32 devices in a mesh: table: 4 (over y, core), batch: 8 (over z, x).
Axes of the slice: x: 2, y: 2, z: 4, core: 2. Of those that a mesh axis runs over, the one named last changes fastest.
Arguments:
- emb: bfloat16 [4, 262144, 128], P('table', 'batch'), may hold values from -6 to 6
- short_rows: int32 [192, 4, 32], P(('table', 'batch')), may hold values from 0 to 262143
- short_len: int32 [192, 4], P(('table', 'batch')), may hold values from 1 to 32
- short_sample: int32 [192, 4], P(('table', 'batch')), may hold values from 0 to 7, as said below
- long_rows: int32 [64, 4, 512], P(('table', 'batch')), may hold values from 0 to 262143, as said below
- long_len: int32 [64, 4], P(('table', 'batch')), may hold values from 33 to 500, as said below
- long_sample: int32 [64, 4], P(('table', 'batch')), may hold values from 0 to 7, as said below
Outputs:
- pooled: float32 [256, 4, 128], P(('table', 'batch'))
The draws below stay inside these ranges and needn't reach their ends.
Inputs may be any that keep to these rules, and one draw needn't show every extreme that they name: For each block of 6 short bags and 2 long bags with the same j // 6 and j // 2, and each table, short_sample and long_sample together name each of the 8 samples exactly once. `long_sample`: see short_sample. `long_rows`: within one bag no row id stands more than 256 times among the first long_len positions, and in every draw some bag has a row id that stands exactly that often. `long_len`: in every draw some long bag has length 500.
All inputs are finite; a program needn't handle non-finite values.
Results may differ from the reference program's by a relative error of at most 0.0003.
Values sent between devices are 32-bit elements; how exact they have to be, the bound alone decides.
A program may use at most 64 MiB of HBM per device.

```python
import jax
import jax.numpy as jnp
from jax import lax

E = 128
B_DEV = 8
WS = 32
WL = 512
MAXLEN = 500
LONG_DEV = 2
SHORT_DEV = 6
R = 262144
NT = 4
B = 256
DEVICES = 32


def bag_order(key):
    scores = jax.random.randint(jax.random.fold_in(key, 7), (DEVICES, NT, B_DEV), 0, 1 << 20, dtype=jnp.int32)
    scores = scores * B_DEV + jnp.arange(B_DEV, dtype=jnp.int32)
    return jnp.argsort(scores, axis=2).astype(jnp.int32)


def draw_short_sample(key, part):
    order = bag_order(key)[:, :, :SHORT_DEV]
    return jnp.transpose(order, (0, 2, 1)).reshape(DEVICES * SHORT_DEV, NT)


def draw_long_sample(key, part):
    order = bag_order(key)[:, :, SHORT_DEV:]
    return jnp.transpose(order, (0, 2, 1)).reshape(DEVICES * LONG_DEV, NT)


def long_bags(key):
    bag_count = DEVICES * LONG_DEV
    total = bag_count * NT
    ceiling = min(256, MAXLEN)
    middle_low = min(17, ceiling)
    middle_high = min(255, ceiling)
    base = jax.random.fold_in(key, 11)
    lengths = jax.random.randint(jax.random.fold_in(base, 1), (bag_count, NT), WS + 1, MAXLEN + 1, dtype=jnp.int32)
    bag_rank = jax.random.permutation(jax.random.fold_in(base, 2), total).astype(jnp.int32).reshape(bag_count, NT)
    middle = jax.random.randint(jax.random.fold_in(base, 3), (bag_count, NT), middle_low, middle_high + 1, dtype=jnp.int32)
    repeats = jnp.where(bag_rank == 0, ceiling, jnp.where(bag_rank <= 15, middle, 0)).astype(jnp.int32)
    lengths = jnp.where(bag_rank == 0, MAXLEN, jnp.maximum(lengths, repeats)).astype(jnp.int32)
    chosen = jax.random.randint(jax.random.fold_in(base, 4), (bag_count, NT), 0, R, dtype=jnp.int32)
    others = jax.random.randint(jax.random.fold_in(base, 5), (bag_count, NT, WL), 0, R - 1, dtype=jnp.int32)
    others = (chosen[:, :, None] + 1 + others) % R
    place = jnp.arange(WL, dtype=jnp.int32)[None, None, :]
    scores = jax.random.randint(jax.random.fold_in(base, 6), (bag_count, NT, WL), 0, 1 << 20, dtype=jnp.int32)
    scores = scores * WL + place
    scores = jnp.where(place < lengths[:, :, None], scores, scores + (1 << 30))
    order = jnp.argsort(scores, axis=2).astype(jnp.int32)
    position_rank = jnp.argsort(order, axis=2).astype(jnp.int32)
    rows = jnp.where(position_rank < repeats[:, :, None], chosen[:, :, None], others)
    return (rows.astype(jnp.int32), lengths.astype(jnp.int32))


def draw_long_rows(key, part):
    return long_bags(key)[0]


def draw_long_len(key, part):
    return long_bags(key)[1]


def plant(entries, rng, least, largest):
    dims = entries.shape
    spot = [jax.random.randint(jax.random.fold_in(rng, axis), (), 0, dims[axis]) for axis in range(len(dims))]
    entries = entries.at[tuple(spot)].set(least)
    longest = dims.index(max(dims))
    spot[longest] = (spot[longest] + 1) % dims[longest]
    return entries.at[tuple(spot)].set(largest)


def levels(own_key, dims, split, low, high):
    level, own = 1.0, jax.random.fold_in(own_key, 6)
    for dim, parts in split:
        steps = jnp.exp(jax.random.uniform(jax.random.fold_in(own, dim), (parts,), jnp.float32, low / len(split), high / len(split)))
        level = level * jnp.repeat(steps, dims[dim] // parts).reshape([-1 if axis == dim else 1 for axis in range(len(dims))])
    return level


def noise(own_key, shape, scale, reach, cuts=(), kind=jnp.bfloat16):
    result = jax.random.normal(own_key, shape, jnp.float32) * scale
    if len(cuts) > 0:
        result = levels(own_key, shape, cuts, -0.22, 0.18) * result
    return jnp.clip(result, min=-reach, max=reach).astype(kind)


def setup_inputs(seed: int = 0) -> dict:
    seeds = jax.random.split(jax.random.key(seed), 8)
    emb = noise(seeds[0], (NT, R, E), 1.0, 6.0, ((0, 4), (1, 8)))
    short_rows = plant(jax.random.randint(seeds[1], (DEVICES * SHORT_DEV, NT, WS), 0, R), jax.random.fold_in(seeds[1], 1), 0, R - 1).astype(jnp.int32)
    short_len = plant(jax.random.randint(seeds[2], (DEVICES * SHORT_DEV, NT), 1, WS + 1), jax.random.fold_in(seeds[2], 1), 1, WS).astype(jnp.int32)
    short_sample = draw_short_sample(jax.random.fold_in(seeds[7], 71), 0)
    long_rows = draw_long_rows(jax.random.fold_in(seeds[7], 71), 0)
    long_len = draw_long_len(jax.random.fold_in(seeds[7], 71), 0)
    long_sample = draw_long_sample(jax.random.fold_in(seeds[7], 71), 0)
    return {"emb": emb, "short_rows": short_rows, "short_len": short_len, "short_sample": short_sample, "long_rows": long_rows, "long_len": long_len, "long_sample": long_sample}


def bag_sums(table, rows, lengths):
    place = jnp.arange(rows.shape[1], dtype=jnp.int32)
    valid = place[None, :] < lengths[:, None]
    picked = table[rows].astype(jnp.float32)
    total = lax.optimization_barrier(jnp.sum(jnp.where(valid[:, :, None], picked, jnp.float32(0.0)), axis=1))
    return total / jnp.sqrt(lengths.astype(jnp.float32))[:, None]

def reference(emb, short_rows, short_len, short_sample, long_rows, long_len, long_sample):
    pooled = jnp.zeros((B, NT, E), jnp.float32)
    short_owner = jnp.arange(DEVICES * SHORT_DEV, dtype=jnp.int32) // SHORT_DEV * B_DEV
    long_owner = jnp.arange(DEVICES * LONG_DEV, dtype=jnp.int32) // LONG_DEV * B_DEV
    for table_id in range(NT):
        short_vec = bag_sums(emb[table_id], short_rows[:, table_id, :], short_len[:, table_id])
        pooled = pooled.at[short_owner + short_sample[:, table_id], table_id].set(short_vec)
        long_vec = bag_sums(emb[table_id], long_rows[:, table_id, :], long_len[:, table_id])
        pooled = pooled.at[long_owner + long_sample[:, table_id], table_id].set(long_vec)
    return pooled
```

```python
import functools
import math

import jax
import jax.numpy as jnp
from jax import lax
from jax.experimental import pallas as pl
from jax.experimental.pallas import tpu as pltpu
from jax.sharding import PartitionSpec as P

MESH = pl.DeviceIdType.MESH
LANES = 128
GROUP = 8
EARLIER = 4096
TABLE_CHUNKS = 8
CONVERT_ROWS = 256


def capacity_of(short_dev, short_width, long_dev, long_width, batch):
    mean = (short_dev * short_width + long_dev * long_width) / batch
    slots = math.ceil((mean + 3.2 * math.sqrt(mean)) / 16) * 16
    return slots - 16 if slots % LANES == 0 else slots


def pool_kernel(
    tables,
    batch,
    slots,
    round_ref,
    emb_ref,
    short_rows_ref,
    short_len_ref,
    short_sample_ref,
    long_rows_ref,
    long_len_ref,
    long_sample_ref,
    out_ref,
    flag_ref,
    table_raw,
    table,
    long_ids,
    long_count,
    send_ids,
    send_weights,
    recv_ids,
    recv_weights,
    picked,
    send_sums,
    recv_sums,
    table_sems,
    own_sem,
    send_sems,
    ids_sems,
    weights_sems,
    sums_sem,
):
    devices = tables * batch
    short_dev, _, short_width = short_rows_ref.shape
    long_dev, _, long_width = long_rows_ref.shape
    rows_dev = table.shape[0]
    samples = out_ref.shape[0]
    halves = pl.cdiv(slots, LANES)
    groups = devices // GROUP
    my_table = lax.axis_index("table")
    my_batch = lax.axis_index("batch")
    me = my_table * batch + my_batch

    def peer(index):
        return (index // batch, index % batch)

    chunk = rows_dev // TABLE_CHUNKS

    def table_copy(index):
        span = pl.ds(index * chunk, chunk)
        return pltpu.make_async_copy(
            emb_ref.at[0, span, :], table_raw.at[span, :], table_sems.at[index]
        )

    for index in range(TABLE_CHUNKS):
        table_copy(index).start()

    barrier = pltpu.get_barrier_semaphore()

    def greet(step, _):
        pl.semaphore_signal(
            barrier, inc=1, device_id=peer((me + step) % devices), device_id_type=MESH
        )
        return 0

    lax.fori_loop(1, devices, greet, 0)

    pieces = long_width // LANES
    table_place = lax.broadcasted_iota(jnp.int32, (tables, long_width), 0)
    place = lax.broadcasted_iota(jnp.int32, (tables, long_width), 1)
    for bag in range(long_dev):
        lengths = jnp.zeros((tables, long_width), jnp.int32)
        for k in range(tables):
            lengths = jnp.where(table_place == k, long_len_ref[bag, k], lengths)
        masked = jnp.where(place < lengths, long_rows_ref[bag], -1)
        for c in range(pieces):
            long_ids[pl.ds(bag * tables, tables), c, :] = masked[:, c * LANES : (c + 1) * LANES]

    sub8 = lax.broadcasted_iota(jnp.int32, (8, LANES), 0)
    lane8 = lax.broadcasted_iota(jnp.int32, (8, LANES), 1)

    def merge(bag, _):
        row = long_ids[bag]
        parts = [row[c : c + 1, :] for c in range(pieces)]
        wide = [jnp.broadcast_to(part, (8, LANES)) for part in parts]
        total = [jnp.zeros((8, LANES), jnp.int32) for _ in range(pieces)]
        for c in range(pieces):
            column = jnp.broadcast_to(parts[c], (LANES, LANES)).T
            for g in range(LANES // 8):
                other = column[g * 8 : (g + 1) * 8, :]
                diagonal = jnp.where(sub8 + g * 8 < lane8, EARLIER + 1, 1)
                for e in range(pieces):
                    weight = diagonal if e == c else (EARLIER + 1 if c < e else 1)
                    total[e] = total[e] + jnp.where(other == wide[e], weight, 0)
        for e in range(pieces):
            seen = jnp.sum(total[e], axis=0, keepdims=True)
            keep = (seen < EARLIER) & (parts[e] >= 0)
            long_count[bag, pl.ds(e, 1), :] = jnp.where(keep, seen, 0)
        return 0

    lax.fori_loop(0, long_dev * tables, merge, 0)

    skipped = (round_ref[0] * slots).astype(jnp.float32)
    lane1 = lax.broadcasted_iota(jnp.int32, (1, LANES), 1)
    shard_base = lax.broadcasted_iota(jnp.int32, (batch, LANES), 0) * rows_dev
    slot_column = lax.broadcasted_iota(jnp.int32, (LANES, LANES), 0)
    first = lax.broadcasted_iota(jnp.int32, (LANES, 2 * LANES), 0)
    second = lax.broadcasted_iota(jnp.int32, (LANES, 2 * LANES), 1)
    prefix = ((first < second) | (second >= LANES)).astype(jnp.float32).astype(jnp.bfloat16)
    per_chunk = LANES // short_width
    short_chunks = pl.cdiv(short_dev, per_chunk)
    short_planes = []
    for c in range(short_chunks):
        planes = [
            short_rows_ref[c * per_chunk + i]
            if c * per_chunk + i < short_dev
            else jnp.full((tables, short_width), -1, jnp.int32)
            for i in range(per_chunk)
        ]
        short_planes.append(jnp.concatenate(planes, axis=1))

    over = jnp.zeros((batch, LANES), jnp.float32)
    results = []
    for k in range(tables):
        entries = []
        for bag in range(long_dev):
            for c in range(pieces):
                at = (bag * tables + k, slice(c, c + 1), slice(None))
                sample = jnp.full((1, LANES), long_sample_ref[bag, k], jnp.int32)
                entries.append((long_ids[at], long_count[at], sample))
        for c in range(short_chunks):
            lengths = jnp.zeros((1, LANES), jnp.int32)
            sample = jnp.zeros((1, LANES), jnp.int32)
            for i in range(per_chunk):
                bag = c * per_chunk + i
                if bag < short_dev:
                    mine = lane1 // short_width == i
                    lengths = jnp.where(mine, short_len_ref[bag, k], lengths)
                    sample = jnp.where(mine, short_sample_ref[bag, k], sample)
            count = jnp.where(lane1 % short_width < lengths, 1, 0)
            entries.append((short_planes[c][k : k + 1, :], count, sample))

        inside, local = [], []
        for ids, count, _ in entries:
            here = ids - shard_base
            local.append(here)
            inside.append((here >= 0) & (here < rows_dev) & (count > 0))
        marks = jnp.concatenate(
            [jnp.where(m, 1.0, 0.0).astype(jnp.float32) for m in inside], axis=0
        ).astype(jnp.bfloat16)
        ranks = jnp.dot(marks, prefix, preferred_element_type=jnp.float32)
        offset = jnp.zeros((batch, LANES), jnp.float32) - skipped
        left, right = [], []
        for c, (_, count, sample) in enumerate(entries):
            block = ranks[c * batch : (c + 1) * batch, :]
            rank = block[:, :LANES] + offset
            offset = offset + block[:, LANES:]
            over = jnp.maximum(over, jnp.where(inside[c] & (rank >= slots), 1.0, 0.0))
            target = jnp.zeros((batch, LANES), jnp.float32)
            masks = []
            for h in range(halves):
                top = min(slots, (h + 1) * LANES)
                mask = inside[c] & (rank >= h * LANES) & (rank < top)
                masks.append(mask)
                target = jnp.where(mask, rank - h * LANES, target)
            target = jnp.sum(target, axis=0, keepdims=True).astype(jnp.int32)
            right.append(
                jnp.where(slot_column == target, 1.0, 0.0).astype(jnp.bfloat16)
            )
            values = [
                (local[c] >> 8).astype(jnp.float32),
                (local[c] & 255).astype(jnp.float32),
                jnp.broadcast_to(sample.astype(jnp.float32), (batch, LANES)),
                jnp.broadcast_to(count.astype(jnp.float32), (batch, LANES)),
            ]
            left.append(
                jnp.concatenate(
                    [jnp.where(m, v, 0.0) for v in values for m in masks], axis=0
                ).astype(jnp.bfloat16)
            )
        results.append(
            lax.dot_general(
                jnp.concatenate(left, axis=1),
                jnp.concatenate(right, axis=1),
                (((1,), (1,)), ((), ())),
                preferred_element_type=jnp.float32,
            )
        )

    overflow = jnp.max(over, axis=(0, 1), keepdims=True).astype(jnp.int32)
    for k in range(tables):
        values = [
            [results[k][(p * halves + h) * batch :][:batch] for h in range(halves)]
            for p in range(4)
        ]
        span = pl.ds(k * batch, batch)
        for h in range(halves):
            ids = (values[0][h] * 256.0 + values[1][h]).astype(jnp.int32)
            send_ids[span, h, :] = jnp.clip(ids, 0, rows_dev - 1)
            send_weights[span, h, :] = values[2][h].astype(jnp.int32)
            count = values[3][h].astype(jnp.int32)
            if h == halves - 1:
                count = jnp.where(lane1 == LANES - 1, overflow, count)
            send_weights[span, halves + h, :] = count

    pl.semaphore_wait(barrier, devices - 1)

    def ids_copy(step):
        target = (me + step) % devices
        return pltpu.make_async_remote_copy(
            src_ref=send_ids.at[target],
            dst_ref=recv_ids.at[step],
            send_sem=send_sems.at[0],
            recv_sem=ids_sems.at[step // GROUP],
            device_id=peer(target),
            device_id_type=MESH,
        )

    def weights_copy(step):
        target = (me + step) % devices
        return pltpu.make_async_remote_copy(
            src_ref=send_weights.at[target],
            dst_ref=recv_weights.at[step],
            send_sem=send_sems.at[1],
            recv_sem=weights_sems.at[step // GROUP],
            device_id=peer(target),
            device_id_type=MESH,
        )

    own_ids = pltpu.make_async_copy(send_ids.at[me], recv_ids.at[0], own_sem)
    own_ids.start()
    recv_weights[0] = send_weights[me]

    def send(step, _):
        ids_copy(step).start()
        weights_copy(step).start()
        return 0

    lax.fori_loop(1, devices, send, 0)

    for index in range(TABLE_CHUNKS):
        table_copy(index).wait()

        def widen(step, _):
            span = pl.ds(
                pl.multiple_of(index * chunk + step * CONVERT_ROWS, CONVERT_ROWS), CONVERT_ROWS
            )
            table[span, :] = table_raw[span, :].astype(jnp.float32)
            return 0

        lax.fori_loop(0, chunk // CONVERT_ROWS, widen, 0)

    own_ids.wait()

    sample_rows = lax.broadcasted_iota(jnp.int32, (samples, LANES), 0)
    for group in range(groups):
        begin = group * GROUP
        arriving = GROUP - 1 if group == 0 else GROUP
        pltpu.make_async_copy(
            recv_ids.at[pl.ds(0, arriving)], recv_ids.at[pl.ds(0, arriving)], ids_sems.at[group]
        ).wait()

        def pick(step, _):
            for slot in range(slots):
                row = recv_ids[begin + step, slot // LANES, slot % LANES]
                picked[step, pl.ds(slot, 1), :] = table[pl.ds(row, 1), :]
            return 0

        lax.fori_loop(0, GROUP, pick, 0)
        pltpu.make_async_copy(
            recv_weights.at[pl.ds(0, arriving)],
            recv_weights.at[pl.ds(0, arriving)],
            weights_sems.at[group],
        ).wait()
        for step in range(GROUP):
            weights = []
            for h in range(halves):
                sample = recv_weights[begin + step, pl.ds(h, 1), :]
                count = recv_weights[begin + step, pl.ds(halves + h, 1), :]
                weight = jnp.where(sample_rows == sample, count, 0).astype(jnp.float32)
                weights.append(weight[:, : min(LANES, slots - h * LANES)])
            send_sums[begin + step] = jnp.dot(
                jnp.concatenate(weights, axis=1).astype(jnp.bfloat16),
                picked[step].astype(jnp.bfloat16),
                preferred_element_type=jnp.float32,
            )

        def answer(step, _):
            target = (me - step + devices) % devices
            pltpu.make_async_remote_copy(
                src_ref=send_sums.at[step],
                dst_ref=recv_sums.at[me],
                send_sem=send_sems.at[2],
                recv_sem=sums_sem,
                device_id=peer(target),
                device_id_type=MESH,
            ).start()
            return 0

        if group == 0:
            recv_sums[me] = send_sums[0]
        lax.fori_loop(max(begin, 1), begin + GROUP, answer, 0)

    others = pl.ds(0, devices - 1)
    pltpu.make_async_copy(recv_sums.at[others], recv_sums.at[others], sums_sem).wait()

    last = recv_weights[0, pl.ds(2 * halves - 1, 1), :]
    for step in range(1, devices):
        last = jnp.maximum(last, recv_weights[step, pl.ds(2 * halves - 1, 1), :])
    flag_ref[0] = jnp.max(jnp.where(lane1 == LANES - 1, last, 0))

    for k in range(tables):
        total = recv_sums[k * batch]
        for s in range(1, batch):
            total = total + recv_sums[k * batch + s]
        lengths = jnp.zeros((samples, LANES), jnp.int32)
        for bag in range(short_dev):
            lengths = jnp.where(
                sample_rows == short_sample_ref[bag, k], short_len_ref[bag, k], lengths
            )
        for bag in range(long_dev):
            lengths = jnp.where(
                sample_rows == long_sample_ref[bag, k], long_len_ref[bag, k], lengths
            )
        out_ref[:, k, :] = total / jnp.sqrt(lengths.astype(jnp.float32))

    pltpu.make_async_copy(send_ids.at[others], send_ids.at[others], send_sems.at[0]).wait()
    pltpu.make_async_copy(
        send_weights.at[others], send_weights.at[others], send_sems.at[1]
    ).wait()
    pltpu.make_async_copy(send_sums.at[others], send_sums.at[others], send_sems.at[2]).wait()


def on_device(emb, short_rows, short_len, short_sample, long_rows, long_len, long_sample):
    tables = lax.axis_size("table")
    batch = lax.axis_size("batch")
    devices = tables * batch
    short_dev, _, short_width = short_rows.shape
    long_dev, _, long_width = long_rows.shape
    rows_dev, width = emb.shape[1:]
    samples = short_dev + long_dev
    slots = capacity_of(short_dev, short_width, long_dev, long_width, batch)
    halves = pl.cdiv(slots, LANES)
    assert width == LANES and rows_dev <= 65536 and rows_dev % (TABLE_CHUNKS * CONVERT_ROWS) == 0
    assert long_width % LANES == 0 and long_width < EARLIER and LANES % short_width == 0
    assert devices % GROUP == 0

    smem = pl.BlockSpec(memory_space=pltpu.SMEM)
    vmem = pl.BlockSpec(memory_space=pltpu.VMEM)
    call = pl.pallas_call(
        functools.partial(pool_kernel, tables, batch, slots),
        out_shape=(
            jax.ShapeDtypeStruct((samples, tables, width), jnp.float32),
            jax.ShapeDtypeStruct((1,), jnp.int32),
        ),
        in_specs=[smem, pl.BlockSpec(memory_space=pl.ANY), vmem, smem, smem, vmem, smem, smem],
        out_specs=(vmem, smem),
        scratch_shapes=[
            pltpu.VMEM((rows_dev, width), jnp.bfloat16),
            pltpu.VMEM((rows_dev, width), jnp.float32),
            pltpu.VMEM((long_dev * tables, long_width // LANES, LANES), jnp.int32),
            pltpu.VMEM((long_dev * tables, long_width // LANES, LANES), jnp.int32),
            pltpu.VMEM((devices, halves, LANES), jnp.int32),
            pltpu.VMEM((devices, 2 * halves, LANES), jnp.int32),
            pltpu.SMEM((devices, halves, LANES), jnp.int32),
            pltpu.VMEM((devices, 2 * halves, LANES), jnp.int32),
            pltpu.VMEM((GROUP, slots, width), jnp.float32),
            pltpu.VMEM((devices, samples, width), jnp.float32),
            pltpu.VMEM((devices, samples, width), jnp.float32),
            pltpu.SemaphoreType.DMA((TABLE_CHUNKS,)),
            pltpu.SemaphoreType.DMA,
            pltpu.SemaphoreType.DMA((3,)),
            pltpu.SemaphoreType.DMA((devices // GROUP,)),
            pltpu.SemaphoreType.DMA((devices // GROUP,)),
            pltpu.SemaphoreType.DMA,
        ],
        compiler_params=pltpu.CompilerParams(
            collective_id=0, has_side_effects=True, vmem_limit_bytes=56 * 2**20
        ),
        name="pool",
    )

    def run(index):
        return call(
            jnp.full((1,), index, jnp.int32),
            emb,
            short_rows,
            short_len,
            short_sample,
            long_rows,
            long_len,
            long_sample,
        )

    rounds = pl.cdiv(short_dev * short_width + long_dev * long_width, slots)
    pooled, flag = run(0)
    return lax.cond(
        flag[0] > 0,
        lambda value: lax.fori_loop(1, rounds, lambda r, acc: acc + run(r)[0], value),
        lambda value: value,
        pooled,
    )


def solution(mesh):
    return jax.shard_map(
        on_device,
        mesh=mesh,
        in_specs=(
            P("table", "batch", None),
            P(("table", "batch"), None, None),
            P(("table", "batch"), None),
            P(("table", "batch"), None),
            P(("table", "batch"), None, None),
            P(("table", "batch"), None),
            P(("table", "batch"), None),
        ),
        out_specs=P(("table", "batch"), None, None),
        check_vma=False,
    )
```

```python
import functools
import math

import jax
import jax.numpy as jnp
from jax import lax
from jax.experimental import pallas as pl
from jax.experimental.pallas import tpu as pltpu
from jax.sharding import PartitionSpec as P

MESH = pl.DeviceIdType.MESH
LANES = 128
GROUP = 8
TABLE_CHUNKS = 8
CONVERT_ROWS = 512


def capacity_of(short_dev, short_width, long_dev, long_width, batch):
    mean = (short_dev * short_width + long_dev * long_width) / batch
    slots = math.ceil((mean + 3.2 * math.sqrt(mean)) / 16) * 16
    return slots - 16 if slots % LANES == 0 else slots


def pool_kernel(
    tables,
    batch,
    slots,
    round_ref,
    emb_ref,
    short_rows_hbm,
    short_len_hbm,
    short_sample_hbm,
    long_rows_hbm,
    long_len_hbm,
    long_sample_hbm,
    out_ref,
    flag_ref,
    short_rows_ref,
    short_len_ref,
    short_sample_ref,
    long_rows_ref,
    long_len_ref,
    long_sample_ref,
    table_raw,
    table,
    send_ids,
    send_weights,
    recv_ids,
    recv_weights,
    picked,
    send_sums,
    recv_sums,
    input_sems,
    table_sems,
    send_sems,
    ids_sems,
    weights_sems,
    sums_sem,
):
    devices = tables * batch
    short_dev, _, short_width = short_rows_ref.shape
    long_dev, _, long_width = long_rows_ref.shape
    rows_dev = table.shape[0]
    samples = out_ref.shape[0]
    halves = pl.cdiv(slots, LANES)
    groups = devices // GROUP
    my_table = lax.axis_index("table")
    my_batch = lax.axis_index("batch")
    me = my_batch * tables + my_table

    def partner(step):
        return my_table ^ (step % tables), my_batch ^ (step // tables)

    chunk = rows_dev // TABLE_CHUNKS

    def table_copy(index):
        span = pl.ds(index * chunk, chunk)
        return pltpu.make_async_copy(
            emb_ref.at[0, span, :], table_raw.at[span, :], table_sems.at[index]
        )

    inputs = [
        pltpu.make_async_copy(source, target, input_sems.at[index])
        for index, (source, target) in enumerate(
            [
                (long_rows_hbm, long_rows_ref),
                (long_len_hbm, long_len_ref),
                (short_rows_hbm, short_rows_ref),
                (short_len_hbm, short_len_ref),
                (short_sample_hbm, short_sample_ref),
                (long_sample_hbm, long_sample_ref),
            ]
        )
    ]
    for copy in inputs:
        copy.start()
    barrier = pltpu.get_barrier_semaphore()
    for step in reversed(range(1, devices)):
        pl.semaphore_signal(barrier, inc=1, device_id=partner(step), device_id_type=MESH)
    for index in range(TABLE_CHUNKS):
        table_copy(index).start()
    for copy in inputs:
        copy.wait()

    pieces = long_width // LANES
    table_place = lax.broadcasted_iota(jnp.int32, (tables, long_width), 0)
    place = lax.broadcasted_iota(jnp.int32, (tables, long_width), 1)
    sub8 = lax.broadcasted_iota(jnp.int32, (8, LANES), 0)
    lane8 = lax.broadcasted_iota(jnp.int32, (8, LANES), 1)
    ones = jnp.ones((8, LANES), jnp.float32).astype(jnp.bfloat16)
    long_entries = [[] for _ in range(tables)]
    for bag in range(long_dev):
        lengths = jnp.zeros((tables, long_width), jnp.int32)
        for k in range(tables):
            lengths = jnp.where(table_place == k, long_len_ref[bag, k], lengths)
        masked = jnp.where(place < lengths, long_rows_ref[bag], -1)
        for k in range(tables):
            parts = [masked[k : k + 1, c * LANES : (c + 1) * LANES] for c in range(pieces)]
            wide = [jnp.broadcast_to(part, (8, LANES)) for part in parts]
            column = jnp.broadcast_to(parts[0], (LANES, LANES)).T
            before = [jnp.zeros((8, LANES), jnp.float32) for _ in range(pieces)]
            equal = []
            for g in range(LANES // 8):
                other = column[g * 8 : (g + 1) * 8, :]
                row = None
                for e in range(pieces):
                    same = jnp.where(other == wide[e], 1.0, 0.0)
                    row = same if row is None else row + same
                    if e == 0:
                        same = jnp.where(sub8 + g * 8 < lane8, same, 0.0)
                    before[e] = before[e] + same
                equal.append(row)
            count = lax.dot_general(
                ones,
                jnp.concatenate(equal, axis=0).astype(jnp.bfloat16),
                (((1,), (1,)), ((), ())),
                preferred_element_type=jnp.float32,
            )[0:1, :]
            sample = jnp.full((1, LANES), long_sample_ref[bag, k], jnp.int32).astype(jnp.float32)
            for e in range(pieces):
                keep = jnp.sum(before[e], axis=0, keepdims=True) < 0.5
                total = count if e == 0 else jnp.ones((1, LANES), jnp.float32)
                long_entries[k].append((parts[e], jnp.where(keep, total, 0.0), sample))

    skipped = (round_ref[0] * slots).astype(jnp.float32)
    lane1 = lax.broadcasted_iota(jnp.int32, (1, LANES), 1)
    shard_base = lax.broadcasted_iota(jnp.int32, (batch, LANES), 0) * rows_dev
    slot_column = lax.broadcasted_iota(jnp.int32, (LANES, LANES), 0)
    first = lax.broadcasted_iota(jnp.int32, (LANES, 2 * LANES), 0)
    second = lax.broadcasted_iota(jnp.int32, (LANES, 2 * LANES), 1)
    prefix = ((first < second) | (second >= LANES)).astype(jnp.float32).astype(jnp.bfloat16)
    per_chunk = LANES // short_width
    short_chunks = pl.cdiv(short_dev, per_chunk)
    short_planes = []
    for c in range(short_chunks):
        planes = [
            short_rows_ref[c * per_chunk + i]
            if c * per_chunk + i < short_dev
            else jnp.full((tables, short_width), -1, jnp.int32)
            for i in range(per_chunk)
        ]
        short_planes.append(jnp.concatenate(planes, axis=1))

    over = jnp.zeros((batch, LANES), jnp.float32)
    results = []
    for k in range(tables):
        entries = list(long_entries[k])
        for c in range(short_chunks):
            lengths = jnp.zeros((1, LANES), jnp.int32)
            sample = jnp.zeros((1, LANES), jnp.int32)
            for i in range(per_chunk):
                bag = c * per_chunk + i
                if bag < short_dev:
                    mine = lane1 // short_width == i
                    lengths = jnp.where(mine, short_len_ref[k, bag], lengths)
                    sample = jnp.where(mine, short_sample_ref[k, bag], sample)
            count = jnp.where(lane1 % short_width < lengths, 1.0, 0.0)
            entries.append((short_planes[c][k : k + 1, :], count, sample.astype(jnp.float32)))

        inside, local = [], []
        for ids, count, _ in entries:
            here = ids - shard_base
            local.append(here)
            inside.append((here >= 0) & (here < rows_dev) & (count > 0.0))
        marks = jnp.concatenate(
            [jnp.where(m, 1.0, 0.0).astype(jnp.float32) for m in inside], axis=0
        ).astype(jnp.bfloat16)
        ranks = jnp.dot(marks, prefix, preferred_element_type=jnp.float32)
        offset = jnp.zeros((batch, LANES), jnp.float32) - skipped
        left, right = [], []
        for c, (_, count, sample) in enumerate(entries):
            block = ranks[c * batch : (c + 1) * batch, :]
            rank = block[:, :LANES] + offset
            offset = offset + block[:, LANES:]
            over = jnp.maximum(over, jnp.where(inside[c] & (rank >= slots), 1.0, 0.0))
            target = jnp.zeros((batch, LANES), jnp.float32)
            masks = []
            for h in range(halves):
                top = min(slots, (h + 1) * LANES)
                mask = inside[c] & (rank >= h * LANES) & (rank < top)
                masks.append(mask)
                target = jnp.where(mask, rank - h * LANES, target)
            target = jnp.sum(target, axis=0, keepdims=True).astype(jnp.int32)
            right.append(jnp.where(slot_column == target, 1.0, 0.0).astype(jnp.bfloat16))
            values = [
                (local[c] >> 8).astype(jnp.float32),
                (local[c] & 255).astype(jnp.float32),
                jnp.broadcast_to(sample, (batch, LANES)),
                jnp.broadcast_to(count, (batch, LANES)),
            ]
            left.append(
                jnp.concatenate(
                    [jnp.where(m, v, 0.0) for v in values for m in masks], axis=0
                ).astype(jnp.bfloat16)
            )
        results.append(
            lax.dot_general(
                jnp.concatenate(left, axis=1),
                jnp.concatenate(right, axis=1),
                (((1,), (1,)), ((), ())),
                preferred_element_type=jnp.float32,
            )
        )

    overflow = jnp.max(over, axis=(0, 1), keepdims=True).astype(jnp.int32)
    for k in range(tables):
        values = [
            [results[k][(p * halves + h) * batch :][:batch] for h in range(halves)]
            for p in range(4)
        ]
        for h in range(halves):
            ids = (values[0][h] * 256.0 + values[1][h]).astype(jnp.int32)
            send_ids[:, k, h, :] = jnp.clip(ids, 0, rows_dev - 1)
            send_weights[:, k, h, :] = values[2][h].astype(jnp.int32)
            count = values[3][h].astype(jnp.int32)
            if h == halves - 1:
                count = jnp.where(lane1 == LANES - 1, overflow, count)
            send_weights[:, k, halves + h, :] = count

    pl.semaphore_wait(barrier, devices - 1)
    my_group = me // GROUP
    for step in reversed(range(1, devices)):
        to_table, to_batch = partner(step)
        pltpu.make_async_remote_copy(
            src_ref=send_ids.at[to_batch, to_table],
            dst_ref=recv_ids.at[me],
            send_sem=send_sems.at[0],
            recv_sem=ids_sems.at[my_group],
            device_id=(to_table, to_batch),
            device_id_type=MESH,
        ).start()
    pltpu.make_async_copy(
        send_ids.at[my_batch, my_table], recv_ids.at[me], ids_sems.at[my_group]
    ).start()
    for step in reversed(range(1, devices)):
        to_table, to_batch = partner(step)
        pltpu.make_async_remote_copy(
            src_ref=send_weights.at[to_batch, to_table],
            dst_ref=recv_weights.at[me],
            send_sem=send_sems.at[1],
            recv_sem=weights_sems.at[my_group],
            device_id=(to_table, to_batch),
            device_id_type=MESH,
        ).start()
    recv_weights[me] = send_weights[my_batch, my_table]

    for index in range(TABLE_CHUNKS):
        table_copy(index).wait()

        def widen(step, _):
            span = pl.ds(
                pl.multiple_of(index * chunk + step * CONVERT_ROWS, CONVERT_ROWS), CONVERT_ROWS
            )
            table[span, :] = table_raw[span, :].astype(jnp.float32)
            return 0

        lax.fori_loop(0, chunk // CONVERT_ROWS, widen, 0)

    def arrived(ref, sem, count):
        pltpu.make_async_copy(ref.at[pl.ds(0, count)], ref.at[pl.ds(0, count)], sem).wait()

    sample_rows = lax.broadcasted_iota(jnp.int32, (samples, LANES), 0)
    for group in range(groups):
        begin = group * GROUP
        arrived(recv_ids, ids_sems.at[group], GROUP)
        for step in range(GROUP):
            for slot in range(slots):
                row = recv_ids[begin + step, slot // LANES, slot % LANES]
                picked[group % 2, step, pl.ds(slot, 1), :] = table[pl.ds(row, 1), :]

        @pl.when(my_group == group)
        def _():
            arrived(recv_weights, weights_sems.at[group], GROUP - 1)

        @pl.when(my_group != group)
        def _():
            arrived(recv_weights, weights_sems.at[group], GROUP)

        for step in range(GROUP):
            weights = []
            for h in range(halves):
                sample = recv_weights[begin + step, pl.ds(h, 1), :]
                count = recv_weights[begin + step, pl.ds(halves + h, 1), :]
                weight = jnp.where(sample_rows == sample, count, 0).astype(jnp.float32)
                weights.append(weight[:, : min(LANES, slots - h * LANES)])
            send_sums[begin + step] = jnp.dot(
                jnp.concatenate(weights, axis=1).astype(jnp.bfloat16),
                picked[group % 2, step].astype(jnp.bfloat16),
                preferred_element_type=jnp.float32,
            )
        for step in range(GROUP):
            source = begin + step

            @pl.when(me != source)
            def _():
                pltpu.make_async_remote_copy(
                    src_ref=send_sums.at[source],
                    dst_ref=recv_sums.at[my_batch, my_table],
                    send_sem=send_sems.at[2],
                    recv_sem=sums_sem,
                    device_id=(source % tables, source // tables),
                    device_id_type=MESH,
                ).start()

    recv_sums[my_batch, my_table] = send_sums[me]
    last = recv_weights[0, pl.ds(2 * halves - 1, 1), :]
    for source in range(1, devices):
        last = jnp.maximum(last, recv_weights[source, pl.ds(2 * halves - 1, 1), :])
    flag_ref[0] = jnp.max(jnp.where(lane1 == LANES - 1, last, 0))
    scales = []
    for k in range(tables):
        lengths = jnp.zeros((samples, LANES), jnp.int32)
        for bag in range(short_dev):
            lengths = jnp.where(
                sample_rows == short_sample_ref[k, bag], short_len_ref[k, bag], lengths
            )
        for bag in range(long_dev):
            lengths = jnp.where(
                sample_rows == long_sample_ref[bag, k], long_len_ref[bag, k], lengths
            )
        scales.append(jnp.sqrt(lengths.astype(jnp.float32)))

    arrived(send_sums, sums_sem, devices - 1)

    for k in range(tables):
        total = recv_sums[0, k]
        for s in range(1, batch):
            total = total + recv_sums[s, k]
        out_ref[:, k, :] = total / scales[k]

    arrived(recv_ids, send_sems.at[0], devices - 1)
    arrived(recv_weights, send_sems.at[1], devices - 1)
    arrived(send_sums, send_sems.at[2], devices - 1)


def on_device(emb, short_rows, short_len, short_sample, long_rows, long_len, long_sample):
    tables = lax.axis_size("table")
    batch = lax.axis_size("batch")
    devices = tables * batch
    short_dev, _, short_width = short_rows.shape
    long_dev, _, long_width = long_rows.shape
    rows_dev, width = emb.shape[1:]
    samples = short_dev + long_dev
    slots = capacity_of(short_dev, short_width, long_dev, long_width, batch)
    halves = pl.cdiv(slots, LANES)
    assert width == LANES and rows_dev <= 65536 and rows_dev % (TABLE_CHUNKS * CONVERT_ROWS) == 0
    assert long_width % LANES == 0 and LANES % short_width == 0
    assert devices % GROUP == 0 and tables & (tables - 1) == 0 and batch & (batch - 1) == 0

    smem = pl.BlockSpec(memory_space=pltpu.SMEM)
    vmem = pl.BlockSpec(memory_space=pltpu.VMEM)
    hbm = pl.BlockSpec(memory_space=pl.ANY)
    call = pl.pallas_call(
        functools.partial(pool_kernel, tables, batch, slots),
        out_shape=(
            jax.ShapeDtypeStruct((samples, tables, width), jnp.float32),
            jax.ShapeDtypeStruct((1,), jnp.int32),
        ),
        in_specs=[smem] + [hbm] * 7,
        out_specs=(vmem, smem),
        scratch_shapes=[
            pltpu.VMEM(short_rows.shape, jnp.int32),
            pltpu.SMEM((tables, short_dev), jnp.int32),
            pltpu.SMEM((tables, short_dev), jnp.int32),
            pltpu.VMEM(long_rows.shape, jnp.int32),
            pltpu.SMEM((long_dev, tables), jnp.int32),
            pltpu.SMEM((long_dev, tables), jnp.int32),
            pltpu.VMEM((rows_dev, width), jnp.bfloat16),
            pltpu.VMEM((rows_dev, width), jnp.float32),
            pltpu.VMEM((batch, tables, halves, LANES), jnp.int32),
            pltpu.VMEM((batch, tables, 2 * halves, LANES), jnp.int32),
            pltpu.SMEM((devices, halves, LANES), jnp.int32),
            pltpu.VMEM((devices, 2 * halves, LANES), jnp.int32),
            pltpu.VMEM((2, GROUP, slots, width), jnp.float32),
            pltpu.VMEM((devices, samples, width), jnp.float32),
            pltpu.VMEM((batch, tables, samples, width), jnp.float32),
            pltpu.SemaphoreType.DMA((6,)),
            pltpu.SemaphoreType.DMA((TABLE_CHUNKS,)),
            pltpu.SemaphoreType.DMA((3,)),
            pltpu.SemaphoreType.DMA((devices // GROUP,)),
            pltpu.SemaphoreType.DMA((devices // GROUP,)),
            pltpu.SemaphoreType.DMA,
        ],
        compiler_params=pltpu.CompilerParams(
            collective_id=0, has_side_effects=True, vmem_limit_bytes=56 * 2**20
        ),
        name="pool",
    )

    def run(index):
        return call(
            jnp.full((1,), index, jnp.int32),
            emb,
            short_rows,
            short_len.T,
            short_sample.T,
            long_rows,
            long_len,
            long_sample,
        )

    rounds = pl.cdiv(short_dev * short_width + long_dev * long_width, slots)
    pooled, flag = run(0)
    return lax.cond(
        flag[0] > 0,
        lambda value: lax.fori_loop(1, rounds, lambda r, acc: acc + run(r)[0], value),
        lambda value: value,
        pooled,
    )


def solution(mesh):
    return jax.shard_map(
        on_device,
        mesh=mesh,
        in_specs=(
            P("table", "batch", None),
            P(("table", "batch"), None, None),
            P(("table", "batch"), None),
            P(("table", "batch"), None),
            P(("table", "batch"), None, None),
            P(("table", "batch"), None),
            P(("table", "batch"), None),
        ),
        out_specs=P(("table", "batch"), None, None),
        check_vma=False,
    )
```

```python
import functools
import math

import jax
import jax.numpy as jnp
from jax import lax
from jax._src.lax.control_flow.conditionals import cond_p
from jax.experimental import pallas as pl
from jax.experimental.pallas import tpu as pltpu
from jax.sharding import PartitionSpec as P

MESH = pl.DeviceIdType.MESH
LANES = 128
GROUP = 8
BATCHED = 4
TABLE_CHUNKS = 8
CONVERT_ROWS = 512


def capacity_of(short_dev, short_width, long_dev, long_width, batch):
    mean = (short_dev * short_width + long_dev * long_width) / batch
    slots = math.ceil((mean + 3.2 * math.sqrt(mean)) / 16) * 16
    return slots - 16 if slots % LANES == 0 else slots


def plan_spans(devices):
    spans = []
    for group in range(devices // GROUP):
        begin = group * GROUP
        if group in (1, 2):
            spans += [(begin, BATCHED), (begin + BATCHED, GROUP - BATCHED)]
        else:
            spans.append((begin, GROUP))
    return spans


def pool_kernel(
    tables,
    batch,
    slots,
    round_ref,
    emb_ref,
    short_rows_hbm,
    short_len_hbm,
    short_sample_hbm,
    long_rows_hbm,
    long_len_hbm,
    long_sample_hbm,
    out_ref,
    flag_ref,
    short_rows_ref,
    short_len_ref,
    short_sample_ref,
    long_rows_ref,
    long_len_ref,
    long_sample_ref,
    table_raw,
    table,
    send_ids,
    send_weights,
    recv_ids,
    recv_weights,
    picked,
    send_sums,
    recv_sums,
    flag_out,
    input_sems,
    table_sems,
    send_sems,
    ids_sems,
    weights_sems,
    sums_sem,
    flag_sem,
):
    devices = tables * batch
    short_dev, _, short_width = short_rows_ref.shape
    long_dev, _, long_width = long_rows_ref.shape
    rows_dev = table.shape[0]
    samples = out_ref.shape[0]
    halves = pl.cdiv(slots, LANES)
    my_table = lax.axis_index("table")
    my_batch = lax.axis_index("batch")
    me = my_batch * tables + my_table
    my_group, my_place = me // GROUP, me % GROUP

    def slot_at(step):
        group, place = step // GROUP, step % GROUP
        if group == 0:
            return step
        if group == 1:
            return GROUP + my_place
        return (group // 2 * 2 + my_group % 2) * GROUP + my_place

    def source_of(slot):
        group, place = slot // GROUP, slot % GROUP
        if group == 0:
            return partner(slot)
        if group == 1:
            other = my_group ^ 1
        else:
            other = (my_group // 2 ^ group // 2) * 2 + group % 2
        index = other * GROUP + place
        return index % tables, index // tables

    def partner(step):
        return my_table ^ (step % tables), my_batch ^ (step // tables)

    chunk = rows_dev // TABLE_CHUNKS

    def table_copy(index):
        span = pl.ds(index * chunk, chunk)
        return pltpu.make_async_copy(
            emb_ref.at[0, span, :], table_raw.at[span, :], table_sems.at[index]
        )

    inputs = [
        pltpu.make_async_copy(source, target, input_sems.at[index])
        for index, (source, target) in enumerate(
            [
                (long_rows_hbm, long_rows_ref),
                (long_len_hbm, long_len_ref),
                (short_rows_hbm, short_rows_ref),
                (short_len_hbm, short_len_ref),
                (short_sample_hbm, short_sample_ref),
                (long_sample_hbm, long_sample_ref),
            ]
        )
    ]
    for copy in inputs:
        copy.start()
    barrier = pltpu.get_barrier_semaphore()
    for step in reversed(range(1, devices)):
        pl.semaphore_signal(barrier, inc=1, device_id=partner(step), device_id_type=MESH)
    for index in range(TABLE_CHUNKS):
        table_copy(index).start()
    for copy in inputs:
        copy.wait()

    pieces = long_width // LANES
    table_place = lax.broadcasted_iota(jnp.int32, (tables, long_width), 0)
    place = lax.broadcasted_iota(jnp.int32, (tables, long_width), 1)
    sub8 = lax.broadcasted_iota(jnp.int32, (8, LANES), 0)
    lane8 = lax.broadcasted_iota(jnp.int32, (8, LANES), 1)
    ones = jnp.ones((8, LANES), jnp.float32).astype(jnp.bfloat16)
    long_entries = [[] for _ in range(tables)]
    for bag in range(long_dev):
        lengths = jnp.zeros((tables, long_width), jnp.int32)
        for k in range(tables):
            lengths = jnp.where(table_place == k, long_len_ref[bag, k], lengths)
        masked = jnp.where(place < lengths, long_rows_ref[bag], -1)
        for k in range(tables):
            parts = [masked[k : k + 1, c * LANES : (c + 1) * LANES] for c in range(pieces)]
            wide = [jnp.broadcast_to(part, (8, LANES)) for part in parts]
            column = jnp.broadcast_to(parts[0], (LANES, LANES)).T
            before = [jnp.zeros((8, LANES), jnp.float32) for _ in range(pieces)]
            equal = []
            for g in range(LANES // 8):
                other = column[g * 8 : (g + 1) * 8, :]
                row = None
                for e in range(pieces):
                    same = jnp.where(other == wide[e], 1.0, 0.0)
                    row = same if row is None else row + same
                    if e == 0:
                        same = jnp.where(sub8 + g * 8 < lane8, same, 0.0)
                    before[e] = before[e] + same
                equal.append(row)
            count = lax.dot_general(
                ones,
                jnp.concatenate(equal, axis=0).astype(jnp.bfloat16),
                (((1,), (1,)), ((), ())),
                preferred_element_type=jnp.float32,
            )[0:1, :]
            sample = jnp.full((1, LANES), long_sample_ref[bag, k], jnp.int32).astype(jnp.float32)
            for e in range(pieces):
                keep = jnp.sum(before[e], axis=0, keepdims=True) < 0.5
                total = count if e == 0 else jnp.ones((1, LANES), jnp.float32)
                long_entries[k].append((parts[e], jnp.where(keep, total, 0.0), sample))

    skipped = (round_ref[0] * slots).astype(jnp.float32)
    lane1 = lax.broadcasted_iota(jnp.int32, (1, LANES), 1)
    shard_base = lax.broadcasted_iota(jnp.int32, (batch, LANES), 0) * rows_dev
    slot_column = lax.broadcasted_iota(jnp.int32, (LANES, LANES), 0)
    first = lax.broadcasted_iota(jnp.int32, (LANES, 2 * LANES), 0)
    second = lax.broadcasted_iota(jnp.int32, (LANES, 2 * LANES), 1)
    prefix = ((first < second) | (second >= LANES)).astype(jnp.float32).astype(jnp.bfloat16)
    per_chunk = LANES // short_width
    short_chunks = pl.cdiv(short_dev, per_chunk)
    short_planes = []
    for c in range(short_chunks):
        planes = [
            short_rows_ref[c * per_chunk + i]
            if c * per_chunk + i < short_dev
            else jnp.full((tables, short_width), -1, jnp.int32)
            for i in range(per_chunk)
        ]
        short_planes.append(jnp.concatenate(planes, axis=1))

    over = jnp.zeros((batch, LANES), jnp.float32)
    results = []
    for k in range(tables):
        entries = list(long_entries[k])
        for c in range(short_chunks):
            lengths = jnp.zeros((1, LANES), jnp.int32)
            sample = jnp.zeros((1, LANES), jnp.int32)
            for i in range(per_chunk):
                bag = c * per_chunk + i
                if bag < short_dev:
                    mine = lane1 // short_width == i
                    lengths = jnp.where(mine, short_len_ref[k, bag], lengths)
                    sample = jnp.where(mine, short_sample_ref[k, bag], sample)
            count = jnp.where(lane1 % short_width < lengths, 1.0, 0.0)
            entries.append((short_planes[c][k : k + 1, :], count, sample.astype(jnp.float32)))

        inside, local = [], []
        for ids, count, _ in entries:
            here = ids - shard_base
            local.append(here)
            inside.append((here >= 0) & (here < rows_dev) & (count > 0.0))
        marks = jnp.concatenate(
            [jnp.where(m, 1.0, 0.0).astype(jnp.float32) for m in inside], axis=0
        ).astype(jnp.bfloat16)
        ranks = jnp.dot(marks, prefix, preferred_element_type=jnp.float32)
        offset = jnp.zeros((batch, LANES), jnp.float32) - skipped
        left, right = [], []
        for c, (_, count, sample) in enumerate(entries):
            block = ranks[c * batch : (c + 1) * batch, :]
            rank = block[:, :LANES] + offset
            offset = offset + block[:, LANES:]
            over = jnp.maximum(over, jnp.where(inside[c] & (rank >= slots), 1.0, 0.0))
            target = jnp.zeros((batch, LANES), jnp.float32)
            masks = []
            for h in range(halves):
                top = min(slots, (h + 1) * LANES)
                mask = inside[c] & (rank >= h * LANES) & (rank < top)
                masks.append(mask)
                target = jnp.where(mask, rank - h * LANES, target)
            target = jnp.sum(target, axis=0, keepdims=True).astype(jnp.int32)
            right.append(jnp.where(slot_column == target, 1.0, 0.0).astype(jnp.bfloat16))
            values = [
                (local[c] >> 8).astype(jnp.float32),
                (local[c] & 255).astype(jnp.float32),
                jnp.broadcast_to(sample, (batch, LANES)),
                jnp.broadcast_to(count, (batch, LANES)),
            ]
            left.append(
                jnp.concatenate(
                    [jnp.where(m, v, 0.0) for v in values for m in masks], axis=0
                ).astype(jnp.bfloat16)
            )
        results.append(
            lax.dot_general(
                jnp.concatenate(left, axis=1),
                jnp.concatenate(right, axis=1),
                (((1,), (1,)), ((), ())),
                preferred_element_type=jnp.float32,
            )
        )

    overflow = jnp.max(over, axis=(0, 1), keepdims=True).astype(jnp.int32)
    for k in range(tables):
        values = [
            [results[k][(p * halves + h) * batch :][:batch] for h in range(halves)]
            for p in range(4)
        ]
        for h in range(halves):
            ids = (values[0][h] * 256.0 + values[1][h]).astype(jnp.int32)
            send_ids[:, k, h, :] = jnp.clip(ids, 0, rows_dev - 1)
            send_weights[:, k, h, :] = values[2][h].astype(jnp.int32)
            count = values[3][h].astype(jnp.int32)
            if h == halves - 1:
                count = jnp.where(lane1 == LANES - 1, overflow, count)
            send_weights[:, k, halves + h, :] = count

    pl.semaphore_wait(barrier, devices - 1)
    for step in reversed(range(1, devices)):
        to_table, to_batch = partner(step)
        pltpu.make_async_remote_copy(
            src_ref=send_ids.at[to_batch, to_table],
            dst_ref=recv_ids.at[slot_at(step)],
            send_sem=send_sems.at[0],
            recv_sem=ids_sems.at[slot_at(step) // BATCHED],
            device_id=(to_table, to_batch),
            device_id_type=MESH,
        ).start()
    pltpu.make_async_copy(
        send_ids.at[my_batch, my_table], recv_ids.at[0], ids_sems.at[0]
    ).start()
    for step in reversed(range(1, devices)):
        to_table, to_batch = partner(step)
        pltpu.make_async_remote_copy(
            src_ref=send_weights.at[to_batch, to_table],
            dst_ref=recv_weights.at[slot_at(step)],
            send_sem=send_sems.at[1],
            recv_sem=weights_sems.at[slot_at(step) // BATCHED],
            device_id=(to_table, to_batch),
            device_id_type=MESH,
        ).start()
    recv_weights[0] = send_weights[my_batch, my_table]

    for index in range(TABLE_CHUNKS):
        table_copy(index).wait()

        def widen(step, _):
            span = pl.ds(
                pl.multiple_of(index * chunk + step * CONVERT_ROWS, CONVERT_ROWS), CONVERT_ROWS
            )
            table[span, :] = table_raw[span, :].astype(jnp.float32)
            return 0

        lax.fori_loop(0, chunk // CONVERT_ROWS, widen, 0)

    def arrived(ref, sem, count):
        pltpu.make_async_copy(ref.at[pl.ds(0, count)], ref.at[pl.ds(0, count)], sem).wait()

    sample_rows = lax.broadcasted_iota(jnp.int32, (samples, LANES), 0)
    for group, (begin, size) in enumerate(plan_spans(devices)):
        for first_slot in range(begin, begin + size, BATCHED):
            arrived(recv_ids, ids_sems.at[first_slot // BATCHED], BATCHED)
        for step in range(size):
            for slot in range(slots):
                row = recv_ids[begin + step, slot // LANES, slot % LANES]
                picked[group % 2, step, pl.ds(slot, 1), :] = table[pl.ds(row, 1), :]
        for first_slot in range(begin, begin + size, BATCHED):
            count = BATCHED - 1 if first_slot == 0 else BATCHED
            arrived(recv_weights, weights_sems.at[first_slot // BATCHED], count)

        for step in range(size):
            weights = []
            for h in range(halves):
                sample = recv_weights[begin + step, pl.ds(h, 1), :]
                count = recv_weights[begin + step, pl.ds(halves + h, 1), :]
                weight = jnp.where(sample_rows == sample, count, 0).astype(jnp.float32)
                weights.append(weight[:, : min(LANES, slots - h * LANES)])
            send_sums[begin + step] = jnp.dot(
                jnp.concatenate(weights, axis=1).astype(jnp.bfloat16),
                picked[group % 2, step].astype(jnp.bfloat16),
                preferred_element_type=jnp.float32,
            )
        for step in range(max(begin, 1), begin + size):
            pltpu.make_async_remote_copy(
                src_ref=send_sums.at[step],
                dst_ref=recv_sums.at[my_batch, my_table],
                send_sem=send_sems.at[2],
                recv_sem=sums_sem,
                device_id=source_of(step),
                device_id_type=MESH,
            ).start()

    recv_sums[my_batch, my_table] = send_sums[0]
    last = recv_weights[0, pl.ds(2 * halves - 1, 1), :]
    for source in range(1, devices):
        last = jnp.maximum(last, recv_weights[source, pl.ds(2 * halves - 1, 1), :])
    flag_out[...] = jnp.broadcast_to(jnp.max(jnp.where(lane1 == LANES - 1, last, 0)), (LANES,))
    flag_copy = pltpu.make_async_copy(flag_out, flag_ref, flag_sem)
    flag_copy.start()
    scales = []
    for k in range(tables):
        lengths = jnp.zeros((samples, LANES), jnp.int32)
        for bag in range(short_dev):
            lengths = jnp.where(
                sample_rows == short_sample_ref[k, bag], short_len_ref[k, bag], lengths
            )
        for bag in range(long_dev):
            lengths = jnp.where(
                sample_rows == long_sample_ref[bag, k], long_len_ref[bag, k], lengths
            )
        scales.append(jnp.sqrt(lengths.astype(jnp.float32)))

    arrived(send_sums, sums_sem, devices - 1)

    for k in range(tables):
        total = recv_sums[0, k]
        for s in range(1, batch):
            total = total + recv_sums[s, k]
        out_ref[:, k, :] = total / scales[k]

    flag_copy.wait()
    arrived(recv_ids, send_sems.at[0], devices - 1)
    arrived(recv_weights, send_sems.at[1], devices - 1)
    arrived(send_sums, send_sems.at[2], devices - 1)


def choose(index, first, second, *operands):
    branches = tuple(jax.make_jaxpr(branch)(*operands) for branch in (first, second))
    return cond_p.bind(index, *operands, branches=branches)[0]


def on_device(emb, short_rows, short_len, short_sample, long_rows, long_len, long_sample):
    tables = lax.axis_size("table")
    batch = lax.axis_size("batch")
    devices = tables * batch
    short_dev, _, short_width = short_rows.shape
    long_dev, _, long_width = long_rows.shape
    rows_dev, width = emb.shape[1:]
    samples = short_dev + long_dev
    slots = capacity_of(short_dev, short_width, long_dev, long_width, batch)
    halves = pl.cdiv(slots, LANES)
    assert width == LANES and rows_dev <= 65536 and rows_dev % (TABLE_CHUNKS * CONVERT_ROWS) == 0
    assert long_width % LANES == 0 and LANES % short_width == 0
    assert devices % GROUP == 0 and tables & (tables - 1) == 0 and batch & (batch - 1) == 0

    smem = pl.BlockSpec(memory_space=pltpu.SMEM)
    vmem = pl.BlockSpec(memory_space=pltpu.VMEM)
    hbm = pl.BlockSpec(memory_space=pl.ANY)
    call = pl.pallas_call(
        functools.partial(pool_kernel, tables, batch, slots),
        out_shape=(
            jax.ShapeDtypeStruct((samples, tables, width), jnp.float32),
            pltpu.SMEM((128,), jnp.int32),
        ),
        in_specs=[smem] + [hbm] * 7,
        out_specs=(vmem, hbm),
        scratch_shapes=[
            pltpu.VMEM(short_rows.shape, jnp.int32),
            pltpu.SMEM((tables, short_dev), jnp.int32),
            pltpu.SMEM((tables, short_dev), jnp.int32),
            pltpu.VMEM(long_rows.shape, jnp.int32),
            pltpu.SMEM((long_dev, tables), jnp.int32),
            pltpu.SMEM((long_dev, tables), jnp.int32),
            pltpu.VMEM((rows_dev, width), jnp.bfloat16),
            pltpu.VMEM((rows_dev, width), jnp.float32),
            pltpu.VMEM((batch, tables, halves, LANES), jnp.int32),
            pltpu.VMEM((batch, tables, 2 * halves, LANES), jnp.int32),
            pltpu.SMEM((devices, halves, LANES), jnp.int32),
            pltpu.VMEM((devices, 2 * halves, LANES), jnp.int32),
            pltpu.VMEM((2, GROUP, slots, width), jnp.float32),
            pltpu.VMEM((devices, samples, width), jnp.float32),
            pltpu.VMEM((batch, tables, samples, width), jnp.float32),
            pltpu.VMEM((128,), jnp.int32),
            pltpu.SemaphoreType.DMA((6,)),
            pltpu.SemaphoreType.DMA((TABLE_CHUNKS,)),
            pltpu.SemaphoreType.DMA((3,)),
            pltpu.SemaphoreType.DMA((devices // BATCHED,)),
            pltpu.SemaphoreType.DMA((devices // BATCHED,)),
            pltpu.SemaphoreType.DMA,
            pltpu.SemaphoreType.DMA,
        ],
        compiler_params=pltpu.CompilerParams(
            collective_id=0, has_side_effects=True, vmem_limit_bytes=56 * 2**20
        ),
        name="pool",
    )

    def run(index, operands):
        return call(jnp.reshape(jnp.asarray(index, jnp.int32), (1,)), *operands)

    def rounds(pooled, *operands):
        def again(state):
            index, _, pooled = state
            more, flag = run(index, operands)
            return index + 1, flag[0], pooled + more

        state = (jnp.int32(1), jnp.int32(1), pooled)
        return lax.while_loop(lambda state: state[1] > 0, again, state)[2]

    operands = (emb, short_rows, short_len.T, short_sample.T, long_rows, long_len, long_sample)
    pooled, flag = run(0, operands)
    return choose(flag[0], lambda value, *_: value, rounds, pooled, *operands)


def solution(mesh):
    return jax.shard_map(
        on_device,
        mesh=mesh,
        in_specs=(
            P("table", "batch", None),
            P(("table", "batch"), None, None),
            P(("table", "batch"), None),
            P(("table", "batch"), None),
            P(("table", "batch"), None, None),
            P(("table", "batch"), None),
            P(("table", "batch"), None),
        ),
        out_specs=P(("table", "batch"), None, None),
        check_vma=False,
    )
```

```python
import functools
import math

import jax
import jax.numpy as jnp
from jax import lax
from jax._src.lax.control_flow.conditionals import cond_p
from jax.experimental import pallas as pl
from jax.experimental.pallas import tpu as pltpu
from jax.sharding import PartitionSpec as P

MESH = pl.DeviceIdType.MESH
LANES = 128
INPUTS = 6
GROUP = 8
AHEAD = 2
TABLE_CHUNKS = 2
CONVERT_ROWS = 512


def capacity_of(short_dev, short_width, long_dev, long_width, batch):
    mean = (short_dev * short_width + long_dev * long_width) / batch
    slots = math.ceil((mean + 3.2 * math.sqrt(mean)) / 16) * 16
    return slots - 16 if slots % LANES == 0 else slots


def parts_of(devices):
    parts = [(0, GROUP)]
    for begin in range(GROUP, devices, GROUP):
        parts += [(begin, AHEAD), (begin + AHEAD, GROUP - AHEAD)]
    return parts


def part_at(group, place):
    return 2 * group - (GROUP - 1 - place) // (GROUP - AHEAD)


def plan_spans(devices):
    spans = []
    for group in range(devices // GROUP):
        if group == 0:
            spans.append([0])
        elif group in (1, 2):
            spans += [[2 * group - 1], [2 * group]]
        else:
            spans.append([2 * group - 1, 2 * group])
    return spans


def pool_kernel(
    tables,
    batch,
    slots,
    round_ref,
    emb_ref,
    short_rows_hbm,
    short_len_hbm,
    short_sample_hbm,
    long_rows_hbm,
    long_len_hbm,
    long_sample_hbm,
    out_ref,
    flag_ref,
    short_rows_ref,
    short_len_ref,
    short_sample_ref,
    long_rows_ref,
    long_len_ref,
    long_sample_ref,
    table_raw,
    table,
    send_ids,
    send_weights,
    recv_ids,
    recv_weights,
    picked,
    send_sums,
    recv_sums,
    flag_out,
    local_sems,
    ids_sems,
    weights_sems,
    sums_sem,
):
    devices = tables * batch
    short_dev, _, short_width = short_rows_ref.shape
    long_dev, _, long_width = long_rows_ref.shape
    rows_dev = table.shape[0]
    samples = out_ref.shape[0]
    halves = pl.cdiv(slots, LANES)
    my_table = lax.axis_index("table")
    my_batch = lax.axis_index("batch")
    me = my_batch * tables + my_table
    my_group, my_place = me // GROUP, me % GROUP

    def slot_at(step):
        group, place = step // GROUP, step % GROUP
        if group == 0:
            return step, 0
        if group > 1:
            group = group // 2 * 2 + my_group % 2
        return group * GROUP + my_place, part_at(group, my_place)

    def source_of(slot):
        group, place = slot // GROUP, slot % GROUP
        if group == 0:
            return partner(slot)
        if group == 1:
            other = my_group ^ 1
        else:
            other = (my_group // 2 ^ group // 2) * 2 + group % 2
        index = other * GROUP + place
        return index % tables, index // tables

    def partner(step):
        return my_table ^ (step % tables), my_batch ^ (step // tables)

    chunk = rows_dev // TABLE_CHUNKS

    def table_copy(index):
        span = pl.ds(index * chunk, chunk)
        return pltpu.make_async_copy(
            emb_ref.at[0, span, :], table_raw.at[span, :], local_sems.at[INPUTS + index]
        )

    inputs = [
        pltpu.make_async_copy(source, target, local_sems.at[index])
        for index, (source, target) in enumerate(
            [
                (long_rows_hbm, long_rows_ref),
                (long_len_hbm, long_len_ref),
                (short_rows_hbm, short_rows_ref),
                (short_len_hbm, short_len_ref),
                (short_sample_hbm, short_sample_ref),
                (long_sample_hbm, long_sample_ref),
            ]
        )
    ]
    for copy in inputs:
        copy.start()
    barrier = pltpu.get_barrier_semaphore()
    for step in reversed(range(1, devices)):
        pl.semaphore_signal(barrier, inc=1, device_id=partner(step), device_id_type=MESH)
    for index in range(TABLE_CHUNKS):
        table_copy(index).start()
    for copy in inputs:
        copy.wait()

    pieces = long_width // LANES
    table_place = lax.broadcasted_iota(jnp.int32, (tables, long_width), 0)
    place = lax.broadcasted_iota(jnp.int32, (tables, long_width), 1)
    sub8 = lax.broadcasted_iota(jnp.int32, (8, LANES), 0)
    lane8 = lax.broadcasted_iota(jnp.int32, (8, LANES), 1)
    ones = jnp.ones((8, LANES), jnp.float32).astype(jnp.bfloat16)
    long_entries = [[] for _ in range(tables)]
    for bag in range(long_dev):
        lengths = jnp.zeros((tables, long_width), jnp.int32)
        for k in range(tables):
            lengths = jnp.where(table_place == k, long_len_ref[bag, k], lengths)
        masked = jnp.where(place < lengths, long_rows_ref[bag], -1)
        for k in range(tables):
            parts = [masked[k : k + 1, c * LANES : (c + 1) * LANES] for c in range(pieces)]
            wide = [jnp.broadcast_to(part, (8, LANES)) for part in parts]
            column = jnp.broadcast_to(parts[0], (LANES, LANES)).T
            before = [jnp.zeros((8, LANES), jnp.float32) for _ in range(pieces)]
            equal = []
            for g in range(LANES // 8):
                other = column[g * 8 : (g + 1) * 8, :]
                row = None
                for e in range(pieces):
                    same = jnp.where(other == wide[e], 1.0, 0.0)
                    row = same if row is None else row + same
                    if e == 0:
                        same = jnp.where(sub8 + g * 8 < lane8, same, 0.0)
                    before[e] = before[e] + same
                equal.append(row)
            count = lax.dot_general(
                ones,
                jnp.concatenate(equal, axis=0).astype(jnp.bfloat16),
                (((1,), (1,)), ((), ())),
                preferred_element_type=jnp.float32,
            )[0:1, :]
            sample = jnp.full((1, LANES), long_sample_ref[bag, k], jnp.int32).astype(jnp.float32)
            for e in range(pieces):
                keep = jnp.sum(before[e], axis=0, keepdims=True) < 0.5
                total = count if e == 0 else jnp.ones((1, LANES), jnp.float32)
                long_entries[k].append((parts[e], jnp.where(keep, total, 0.0), sample))

    skipped = (round_ref[0] * slots).astype(jnp.float32)
    lane1 = lax.broadcasted_iota(jnp.int32, (1, LANES), 1)
    shard_base = lax.broadcasted_iota(jnp.int32, (batch, LANES), 0) * rows_dev
    slot_column = lax.broadcasted_iota(jnp.int32, (LANES, LANES), 0)
    first = lax.broadcasted_iota(jnp.int32, (LANES, 2 * LANES), 0)
    second = lax.broadcasted_iota(jnp.int32, (LANES, 2 * LANES), 1)
    prefix = ((first < second) | (second >= LANES)).astype(jnp.float32).astype(jnp.bfloat16)
    per_chunk = LANES // short_width
    short_chunks = pl.cdiv(short_dev, per_chunk)
    short_planes = []
    for c in range(short_chunks):
        planes = [
            short_rows_ref[c * per_chunk + i]
            if c * per_chunk + i < short_dev
            else jnp.full((tables, short_width), -1, jnp.int32)
            for i in range(per_chunk)
        ]
        short_planes.append(jnp.concatenate(planes, axis=1))

    over = jnp.zeros((batch, LANES), jnp.float32)
    results = []
    for k in range(tables):
        entries = list(long_entries[k])
        for c in range(short_chunks):
            lengths = jnp.zeros((1, LANES), jnp.int32)
            sample = jnp.zeros((1, LANES), jnp.int32)
            for i in range(per_chunk):
                bag = c * per_chunk + i
                if bag < short_dev:
                    mine = lane1 // short_width == i
                    lengths = jnp.where(mine, short_len_ref[k, bag], lengths)
                    sample = jnp.where(mine, short_sample_ref[k, bag], sample)
            count = jnp.where(lane1 % short_width < lengths, 1.0, 0.0)
            entries.append((short_planes[c][k : k + 1, :], count, sample.astype(jnp.float32)))

        inside, local = [], []
        for ids, count, _ in entries:
            here = ids - shard_base
            local.append(here)
            inside.append((here >= 0) & (here < rows_dev) & (count > 0.0))
        marks = jnp.concatenate(
            [jnp.where(m, 1.0, 0.0).astype(jnp.float32) for m in inside], axis=0
        ).astype(jnp.bfloat16)
        ranks = jnp.dot(marks, prefix, preferred_element_type=jnp.float32)
        offset = jnp.zeros((batch, LANES), jnp.float32) - skipped
        left, right = [], []
        for c, (_, count, sample) in enumerate(entries):
            block = ranks[c * batch : (c + 1) * batch, :]
            rank = block[:, :LANES] + offset
            offset = offset + block[:, LANES:]
            over = jnp.maximum(over, jnp.where(inside[c] & (rank >= slots), 1.0, 0.0))
            target = jnp.zeros((batch, LANES), jnp.float32)
            masks = []
            for h in range(halves):
                top = min(slots, (h + 1) * LANES)
                mask = inside[c] & (rank >= h * LANES) & (rank < top)
                masks.append(mask)
                target = jnp.where(mask, rank - h * LANES, target)
            target = jnp.sum(target, axis=0, keepdims=True).astype(jnp.int32)
            right.append(jnp.where(slot_column == target, 1.0, 0.0).astype(jnp.bfloat16))
            values = [
                (local[c] >> 8).astype(jnp.float32),
                (local[c] & 255).astype(jnp.float32),
                jnp.broadcast_to(sample, (batch, LANES)),
                jnp.broadcast_to(count, (batch, LANES)),
            ]
            left.append(
                jnp.concatenate(
                    [jnp.where(m, v, 0.0) for v in values for m in masks], axis=0
                ).astype(jnp.bfloat16)
            )
        results.append(
            lax.dot_general(
                jnp.concatenate(left, axis=1),
                jnp.concatenate(right, axis=1),
                (((1,), (1,)), ((), ())),
                preferred_element_type=jnp.float32,
            )
        )

    overflow = jnp.max(over, axis=(0, 1), keepdims=True).astype(jnp.int32)
    for k in range(tables):
        values = [
            [results[k][(p * halves + h) * batch :][:batch] for h in range(halves)]
            for p in range(4)
        ]
        for h in range(halves):
            ids = (values[0][h] * 256.0 + values[1][h]).astype(jnp.int32)
            send_ids[:, k, h, :] = jnp.clip(ids, 0, rows_dev - 1)
            send_weights[:, k, h, :] = values[2][h].astype(jnp.int32)
            count = values[3][h].astype(jnp.int32)
            if h == halves - 1:
                count = jnp.where(lane1 == LANES - 1, overflow, count)
            send_weights[:, k, halves + h, :] = count

    pl.semaphore_wait(barrier, devices - 1)
    def send_to(step, source, target, kind, sems):
        to_table, to_batch = partner(step)
        slot, part = slot_at(step)
        pltpu.make_async_remote_copy(
            src_ref=source.at[to_batch, to_table],
            dst_ref=target.at[slot],
            send_sem=local_sems.at[kind],
            recv_sem=sems.at[part],
            device_id=(to_table, to_batch),
            device_id_type=MESH,
        ).start()

    far = devices - GROUP
    for steps in (range(far, devices), range(1, far)):
        for step in reversed(steps):
            send_to(step, send_ids, recv_ids, 0, ids_sems)
        if 1 in steps:
            pltpu.make_async_copy(
                send_ids.at[my_batch, my_table], recv_ids.at[0], ids_sems.at[0]
            ).start()
        for step in reversed(steps):
            send_to(step, send_weights, recv_weights, 1, weights_sems)
    recv_weights[0] = send_weights[my_batch, my_table]

    for index in range(TABLE_CHUNKS):
        table_copy(index).wait()

        def widen(step, _):
            span = pl.ds(
                pl.multiple_of(index * chunk + step * CONVERT_ROWS, CONVERT_ROWS), CONVERT_ROWS
            )
            table[span, :] = table_raw[span, :].astype(jnp.float32)
            return 0

        lax.fori_loop(0, chunk // CONVERT_ROWS, widen, 0)

    def arrived(ref, sem, count):
        pltpu.make_async_copy(ref.at[pl.ds(0, count)], ref.at[pl.ds(0, count)], sem).wait()

    sample_rows = lax.broadcasted_iota(jnp.int32, (samples, LANES), 0)
    def pick(buffer, slots_of):
        for slot_of in slots_of:
            for slot in range(slots):
                row = recv_ids[slot_of, slot // LANES, slot % LANES]
                picked[buffer, slot_of % GROUP, pl.ds(slot, 1), :] = table[pl.ds(row, 1), :]

    parts = parts_of(devices)

    def wait_ids(span):
        for part in span:
            arrived(recv_ids, ids_sems.at[part], parts[part][1])

    spans = plan_spans(devices)
    started = 0
    for index, span in enumerate(spans):
        begin, size = parts[span[0]][0], sum(parts[part][1] for part in span)
        buffer = index % 2
        if not started:
            wait_ids(span)
        pick(buffer, range(begin + started, begin + size))
        for part in span:
            arrived(recv_weights, weights_sems.at[part], parts[part][1] - (part == 0))

        started = 0
        if index + 1 < len(spans) and 3 not in span and 3 not in spans[index + 1]:
            wait_ids(spans[index + 1])
            following = parts[spans[index + 1][0]][0]
            started = AHEAD
            pick(1 - buffer, range(following, following + started))
        for step in range(begin, begin + size):
            weights = []
            for h in range(halves):
                sample = recv_weights[step, pl.ds(h, 1), :]
                count = recv_weights[step, pl.ds(halves + h, 1), :]
                weight = jnp.where(sample_rows == sample, count, 0).astype(jnp.float32)
                weights.append(weight[:, : min(LANES, slots - h * LANES)])
            send_sums[step] = jnp.dot(
                jnp.concatenate(weights, axis=1).astype(jnp.bfloat16),
                picked[buffer, step % GROUP].astype(jnp.bfloat16),
                preferred_element_type=jnp.float32,
            )
        for step in range(max(begin, 1), begin + size):
            pltpu.make_async_remote_copy(
                src_ref=send_sums.at[step],
                dst_ref=recv_sums.at[my_batch, my_table],
                send_sem=local_sems.at[2],
                recv_sem=sums_sem,
                device_id=source_of(step),
                device_id_type=MESH,
            ).start()

    recv_sums[my_batch, my_table] = send_sums[0]
    last = recv_weights[0, pl.ds(2 * halves - 1, 1), :]
    for source in range(1, devices):
        last = jnp.maximum(last, recv_weights[source, pl.ds(2 * halves - 1, 1), :])
    flag_out[...] = jnp.broadcast_to(jnp.max(jnp.where(lane1 == LANES - 1, last, 0)), (LANES,))
    flag_copy = pltpu.make_async_copy(flag_out, flag_ref, local_sems.at[3])
    flag_copy.start()
    scales = []
    for k in range(tables):
        lengths = jnp.zeros((samples, LANES), jnp.int32)
        for bag in range(short_dev):
            lengths = jnp.where(
                sample_rows == short_sample_ref[k, bag], short_len_ref[k, bag], lengths
            )
        for bag in range(long_dev):
            lengths = jnp.where(
                sample_rows == long_sample_ref[bag, k], long_len_ref[bag, k], lengths
            )
        scales.append(jnp.sqrt(lengths.astype(jnp.float32)))

    arrived(send_sums, sums_sem, devices - 1)

    for k in range(tables):
        total = recv_sums[0, k]
        for s in range(1, batch):
            total = total + recv_sums[s, k]
        out_ref[:, k, :] = total / scales[k]

    flag_copy.wait()
    arrived(recv_ids, local_sems.at[0], devices - 1)
    arrived(recv_weights, local_sems.at[1], devices - 1)
    arrived(send_sums, local_sems.at[2], devices - 1)


def choose(index, first, second, *operands):
    branches = tuple(jax.make_jaxpr(branch)(*operands) for branch in (first, second))
    return cond_p.bind(index, *operands, branches=branches)[0]


def on_device(emb, short_rows, short_len, short_sample, long_rows, long_len, long_sample):
    tables = lax.axis_size("table")
    batch = lax.axis_size("batch")
    devices = tables * batch
    short_dev, _, short_width = short_rows.shape
    long_dev, _, long_width = long_rows.shape
    rows_dev, width = emb.shape[1:]
    samples = short_dev + long_dev
    slots = capacity_of(short_dev, short_width, long_dev, long_width, batch)
    halves = pl.cdiv(slots, LANES)
    assert width == LANES and rows_dev <= 65536 and rows_dev % (TABLE_CHUNKS * CONVERT_ROWS) == 0
    assert long_width % LANES == 0 and LANES % short_width == 0
    assert devices % GROUP == 0 and tables & (tables - 1) == 0 and batch & (batch - 1) == 0

    smem = pl.BlockSpec(memory_space=pltpu.SMEM)
    vmem = pl.BlockSpec(memory_space=pltpu.VMEM)
    hbm = pl.BlockSpec(memory_space=pl.ANY)
    call = pl.pallas_call(
        functools.partial(pool_kernel, tables, batch, slots),
        out_shape=(
            jax.ShapeDtypeStruct((samples, tables, width), jnp.float32),
            pltpu.SMEM((128,), jnp.int32),
        ),
        in_specs=[smem] + [hbm] * 7,
        out_specs=(vmem, hbm),
        scratch_shapes=[
            pltpu.VMEM(short_rows.shape, jnp.int32),
            pltpu.SMEM((tables, short_dev), jnp.int32),
            pltpu.SMEM((tables, short_dev), jnp.int32),
            pltpu.VMEM(long_rows.shape, jnp.int32),
            pltpu.SMEM((long_dev, tables), jnp.int32),
            pltpu.SMEM((long_dev, tables), jnp.int32),
            pltpu.VMEM((rows_dev, width), jnp.bfloat16),
            pltpu.VMEM((rows_dev, width), jnp.float32),
            pltpu.VMEM((batch, tables, halves, LANES), jnp.int32),
            pltpu.VMEM((batch, tables, 2 * halves, LANES), jnp.int32),
            pltpu.SMEM((devices, halves, LANES), jnp.int32),
            pltpu.VMEM((devices, 2 * halves, LANES), jnp.int32),
            pltpu.VMEM((2, GROUP, slots, width), jnp.float32),
            pltpu.VMEM((devices, samples, width), jnp.float32),
            pltpu.VMEM((batch, tables, samples, width), jnp.float32),
            pltpu.VMEM((128,), jnp.int32),
            pltpu.SemaphoreType.DMA((INPUTS + TABLE_CHUNKS,)),
            pltpu.SemaphoreType.DMA((devices // GROUP * 2 - 1,)),
            pltpu.SemaphoreType.DMA((devices // GROUP * 2 - 1,)),
            pltpu.SemaphoreType.DMA,
        ],
        compiler_params=pltpu.CompilerParams(
            collective_id=0, has_side_effects=True, vmem_limit_bytes=56 * 2**20
        ),
        name="pool",
    )

    def run(index, operands):
        return call(jnp.reshape(jnp.asarray(index, jnp.int32), (1,)), *operands)

    def rounds(pooled, *operands):
        def again(state):
            index, _, pooled = state
            more, flag = run(index, operands)
            return index + 1, flag[0], pooled + more

        state = (jnp.int32(1), jnp.int32(1), pooled)
        return lax.while_loop(lambda state: state[1] > 0, again, state)[2]

    operands = (emb, short_rows, short_len.T, short_sample.T, long_rows, long_len, long_sample)
    pooled, flag = run(0, operands)
    return choose(flag[0], lambda value, *_: value, rounds, pooled, *operands)


def solution(mesh):
    return jax.shard_map(
        on_device,
        mesh=mesh,
        in_specs=(
            P("table", "batch", None),
            P(("table", "batch"), None, None),
            P(("table", "batch"), None),
            P(("table", "batch"), None),
            P(("table", "batch"), None, None),
            P(("table", "batch"), None),
            P(("table", "batch"), None),
        ),
        out_specs=P(("table", "batch"), None, None),
        check_vma=False,
    )
```

```python
import functools
import math

import jax
import jax.numpy as jnp
from jax import lax
from jax._src.lax.control_flow.conditionals import cond_p
from jax.experimental import pallas as pl
from jax.experimental.pallas import tpu as pltpu
from jax.sharding import PartitionSpec as P

MESH = pl.DeviceIdType.MESH
LANES = 128
INPUTS = 6
GROUP = 8
AHEAD = 2
TABLE_CHUNKS = 2
CONVERT_ROWS = 512


def capacity_of(short_dev, short_width, long_dev, long_width, batch):
    mean = (short_dev * short_width + long_dev * long_width) / batch
    slots = math.ceil((mean + 3.2 * math.sqrt(mean)) / 16) * 16
    return slots - 16 if slots % LANES == 0 else slots


def parts_of(devices):
    parts = [(0, GROUP)]
    for begin in range(GROUP, devices, GROUP):
        parts += [(begin, AHEAD), (begin + AHEAD, GROUP - AHEAD)]
    return parts


def part_at(group, place):
    return 2 * group - (GROUP - 1 - place) // (GROUP - AHEAD)


def plan_spans(devices):
    spans = []
    for group in range(devices // GROUP):
        if group == 0:
            spans.append([0])
        elif group in (1, 2):
            spans += [[2 * group - 1], [2 * group]]
        else:
            spans.append([2 * group - 1, 2 * group])
    return spans


def pool_kernel(
    tables,
    batch,
    slots,
    round_ref,
    emb_ref,
    short_rows_hbm,
    short_len_hbm,
    short_sample_hbm,
    long_rows_hbm,
    long_len_hbm,
    long_sample_hbm,
    out_ref,
    flag_ref,
    short_rows_ref,
    short_len_ref,
    short_sample_ref,
    long_rows_ref,
    long_len_ref,
    long_sample_ref,
    table_raw,
    table,
    send_ids,
    send_weights,
    recv_ids,
    recv_weights,
    picked,
    send_sums,
    recv_sums,
    flag_out,
    local_sems,
    ids_sems,
    weights_sems,
    sums_sem,
):
    devices = tables * batch
    short_dev, _, short_width = short_rows_ref.shape
    long_dev, _, long_width = long_rows_ref.shape
    rows_dev = table.shape[0]
    samples = out_ref.shape[0]
    halves = pl.cdiv(slots, LANES)
    my_table = lax.axis_index("table")
    my_batch = lax.axis_index("batch")
    me = my_batch * tables + my_table
    my_group, my_place = me // GROUP, me % GROUP

    def slot_at(step):
        group, place = step // GROUP, step % GROUP
        if group == 0:
            return step, 0
        if group > 1:
            group = group // 2 * 2 + my_group % 2
        return group * GROUP + my_place, part_at(group, my_place)

    def source_of(slot):
        group, place = slot // GROUP, slot % GROUP
        if group == 0:
            return partner(slot)
        if group == 1:
            other = my_group ^ 1
        else:
            other = (my_group // 2 ^ group // 2) * 2 + group % 2
        index = other * GROUP + place
        return index % tables, index // tables

    def partner(step):
        return my_table ^ (step % tables), my_batch ^ (step // tables)

    chunk = rows_dev // TABLE_CHUNKS

    def table_copy(index):
        span = pl.ds(index * chunk, chunk)
        return pltpu.make_async_copy(
            emb_ref.at[0, span, :], table_raw.at[span, :], local_sems.at[INPUTS + index]
        )

    inputs = [
        pltpu.make_async_copy(source, target, local_sems.at[index])
        for index, (source, target) in enumerate(
            [
                (long_rows_hbm, long_rows_ref),
                (long_len_hbm, long_len_ref),
                (short_rows_hbm, short_rows_ref),
                (short_len_hbm, short_len_ref),
                (short_sample_hbm, short_sample_ref),
                (long_sample_hbm, long_sample_ref),
            ]
        )
    ]
    barrier = pltpu.get_barrier_semaphore()
    far = devices - GROUP
    for steps in (range(far, devices), range(1, far)):
        for step in reversed(steps):
            pl.semaphore_signal(barrier, inc=1, device_id=partner(step), device_id_type=MESH)
        if far in steps:
            for copy in inputs:
                copy.start()
    for index in range(TABLE_CHUNKS):
        table_copy(index).start()
    for copy in inputs:
        copy.wait()

    pieces = long_width // LANES
    table_place = lax.broadcasted_iota(jnp.int32, (tables, long_width), 0)
    place = lax.broadcasted_iota(jnp.int32, (tables, long_width), 1)
    sub8 = lax.broadcasted_iota(jnp.int32, (8, LANES), 0)
    lane8 = lax.broadcasted_iota(jnp.int32, (8, LANES), 1)
    ones = jnp.ones((8, LANES), jnp.float32).astype(jnp.bfloat16)
    long_entries = [[] for _ in range(tables)]
    for bag in range(long_dev):
        lengths = jnp.zeros((tables, long_width), jnp.int32)
        for k in range(tables):
            lengths = jnp.where(table_place == k, long_len_ref[bag, k], lengths)
        masked = jnp.where(place < lengths, long_rows_ref[bag], -1)
        for k in range(tables):
            parts = [masked[k : k + 1, c * LANES : (c + 1) * LANES] for c in range(pieces)]
            wide = [jnp.broadcast_to(part, (8, LANES)) for part in parts]
            column = jnp.broadcast_to(parts[0], (LANES, LANES)).T
            before = [jnp.zeros((8, LANES), jnp.float32) for _ in range(pieces)]
            equal = []
            for g in range(LANES // 8):
                other = column[g * 8 : (g + 1) * 8, :]
                row = None
                for e in range(pieces):
                    same = jnp.where(other == wide[e], 1.0, 0.0)
                    row = same if row is None else row + same
                    if e == 0:
                        same = jnp.where(sub8 + g * 8 < lane8, same, 0.0)
                    before[e] = before[e] + same
                equal.append(row)
            count = lax.dot_general(
                ones,
                jnp.concatenate(equal, axis=0).astype(jnp.bfloat16),
                (((1,), (1,)), ((), ())),
                preferred_element_type=jnp.float32,
            )[0:1, :]
            sample = jnp.full((1, LANES), long_sample_ref[bag, k], jnp.int32).astype(jnp.float32)
            for e in range(pieces):
                keep = jnp.sum(before[e], axis=0, keepdims=True) < 0.5
                total = count if e == 0 else jnp.ones((1, LANES), jnp.float32)
                long_entries[k].append((parts[e], jnp.where(keep, total, 0.0), sample))

    skipped = (round_ref[0] * slots).astype(jnp.float32)
    lane1 = lax.broadcasted_iota(jnp.int32, (1, LANES), 1)
    shard_base = lax.broadcasted_iota(jnp.int32, (batch, LANES), 0) * rows_dev
    slot_column = lax.broadcasted_iota(jnp.int32, (LANES, LANES), 0)
    first = lax.broadcasted_iota(jnp.int32, (LANES, 2 * LANES), 0)
    second = lax.broadcasted_iota(jnp.int32, (LANES, 2 * LANES), 1)
    prefix = ((first < second) | (second >= LANES)).astype(jnp.float32).astype(jnp.bfloat16)
    per_chunk = LANES // short_width
    short_chunks = pl.cdiv(short_dev, per_chunk)
    short_planes = []
    for c in range(short_chunks):
        planes = [
            short_rows_ref[c * per_chunk + i]
            if c * per_chunk + i < short_dev
            else jnp.full((tables, short_width), -1, jnp.int32)
            for i in range(per_chunk)
        ]
        short_planes.append(jnp.concatenate(planes, axis=1))

    over = jnp.zeros((batch, LANES), jnp.float32)
    results = []
    for k in range(tables):
        entries = list(long_entries[k])
        for c in range(short_chunks):
            lengths = jnp.zeros((1, LANES), jnp.int32)
            sample = jnp.zeros((1, LANES), jnp.int32)
            for i in range(per_chunk):
                bag = c * per_chunk + i
                if bag < short_dev:
                    mine = lane1 // short_width == i
                    lengths = jnp.where(mine, short_len_ref[k, bag], lengths)
                    sample = jnp.where(mine, short_sample_ref[k, bag], sample)
            count = jnp.where(lane1 % short_width < lengths, 1.0, 0.0)
            entries.append((short_planes[c][k : k + 1, :], count, sample.astype(jnp.float32)))

        inside, local = [], []
        for ids, count, _ in entries:
            here = ids - shard_base
            local.append(here)
            inside.append((here >= 0) & (here < rows_dev) & (count > 0.0))
        marks = jnp.concatenate(
            [jnp.where(m, 1.0, 0.0).astype(jnp.float32) for m in inside], axis=0
        ).astype(jnp.bfloat16)
        ranks = jnp.dot(marks, prefix, preferred_element_type=jnp.float32)
        offset = jnp.zeros((batch, LANES), jnp.float32) - skipped
        left, right = [], []
        for c, (_, count, sample) in enumerate(entries):
            block = ranks[c * batch : (c + 1) * batch, :]
            rank = block[:, :LANES] + offset
            offset = offset + block[:, LANES:]
            over = jnp.maximum(over, jnp.where(inside[c] & (rank >= slots), 1.0, 0.0))
            target = jnp.zeros((batch, LANES), jnp.float32)
            masks = []
            for h in range(halves):
                top = min(slots, (h + 1) * LANES)
                mask = inside[c] & (rank >= h * LANES) & (rank < top)
                masks.append(mask)
                target = jnp.where(mask, rank - h * LANES, target)
            target = jnp.sum(target, axis=0, keepdims=True).astype(jnp.int32)
            right.append(jnp.where(slot_column == target, 1.0, 0.0).astype(jnp.bfloat16))
            values = [
                (local[c] >> 8).astype(jnp.float32),
                (local[c] & 255).astype(jnp.float32),
                jnp.broadcast_to(sample, (batch, LANES)),
                jnp.broadcast_to(count, (batch, LANES)),
            ]
            left.append(
                jnp.concatenate(
                    [jnp.where(m, v, 0.0) for v in values for m in masks], axis=0
                ).astype(jnp.bfloat16)
            )
        results.append(
            lax.dot_general(
                jnp.concatenate(left, axis=1),
                jnp.concatenate(right, axis=1),
                (((1,), (1,)), ((), ())),
                preferred_element_type=jnp.float32,
            )
        )

    overflow = jnp.max(over, axis=(0, 1), keepdims=True).astype(jnp.int32)
    for k in range(tables):
        values = [
            [results[k][(p * halves + h) * batch :][:batch] for h in range(halves)]
            for p in range(4)
        ]
        for h in range(halves):
            ids = (values[0][h] * 256.0 + values[1][h]).astype(jnp.int32)
            send_ids[:, k, h, :] = jnp.clip(ids, 0, rows_dev - 1)
            send_weights[:, k, h, :] = values[2][h].astype(jnp.int32)
            count = values[3][h].astype(jnp.int32)
            if h == halves - 1:
                count = jnp.where(lane1 == LANES - 1, overflow, count)
            send_weights[:, k, halves + h, :] = count

    pl.semaphore_wait(barrier, devices - 1)
    def send_to(step, source, target, kind, sems):
        to_table, to_batch = partner(step)
        slot, part = slot_at(step)
        pltpu.make_async_remote_copy(
            src_ref=source.at[to_batch, to_table],
            dst_ref=target.at[slot],
            send_sem=local_sems.at[kind],
            recv_sem=sems.at[part],
            device_id=(to_table, to_batch),
            device_id_type=MESH,
        ).start()

    for steps in (range(far, devices), range(1, far)):
        for step in reversed(steps):
            send_to(step, send_ids, recv_ids, 0, ids_sems)
        if 1 in steps:
            pltpu.make_async_copy(
                send_ids.at[my_batch, my_table], recv_ids.at[0], ids_sems.at[0]
            ).start()
        for step in reversed(steps):
            send_to(step, send_weights, recv_weights, 1, weights_sems)
    recv_weights[0] = send_weights[my_batch, my_table]

    for index in range(TABLE_CHUNKS):
        table_copy(index).wait()

        def widen(step, _):
            span = pl.ds(
                pl.multiple_of(index * chunk + step * CONVERT_ROWS, CONVERT_ROWS), CONVERT_ROWS
            )
            table[span, :] = table_raw[span, :].astype(jnp.float32)
            return 0

        lax.fori_loop(0, chunk // CONVERT_ROWS, widen, 0)

    def arrived(ref, sem, count):
        pltpu.make_async_copy(ref.at[pl.ds(0, count)], ref.at[pl.ds(0, count)], sem).wait()

    sample_rows = lax.broadcasted_iota(jnp.int32, (samples, LANES), 0)
    def pick(buffer, slots_of):
        for slot_of in slots_of:
            for slot in range(slots):
                row = recv_ids[slot_of, slot // LANES, slot % LANES]
                picked[buffer, slot_of % GROUP, pl.ds(slot, 1), :] = table[pl.ds(row, 1), :]

    parts = parts_of(devices)

    def wait_ids(span):
        for part in span:
            arrived(recv_ids, ids_sems.at[part], parts[part][1])

    def multiply(buffer, steps):
        for step in steps:
            weights = []
            for h in range(halves):
                sample = recv_weights[step, pl.ds(h, 1), :]
                count = recv_weights[step, pl.ds(halves + h, 1), :]
                weight = jnp.where(sample_rows == sample, count, 0).astype(jnp.float32)
                weights.append(weight[:, : min(LANES, slots - h * LANES)])
            send_sums[step] = jnp.dot(
                jnp.concatenate(weights, axis=1).astype(jnp.bfloat16),
                picked[buffer, step % GROUP].astype(jnp.bfloat16),
                preferred_element_type=jnp.float32,
            )

    def answer(steps):
        for step in steps:
            if step == 0:
                continue
            pltpu.make_async_remote_copy(
                src_ref=send_sums.at[step],
                dst_ref=recv_sums.at[my_batch, my_table],
                send_sem=local_sems.at[2],
                recv_sem=sums_sem,
                device_id=source_of(step),
                device_id_type=MESH,
            ).start()

    spans = plan_spans(devices)
    started = 0
    for index, span in enumerate(spans):
        begin, size = parts[span[0]][0], sum(parts[part][1] for part in span)
        buffer = index % 2
        if not started:
            wait_ids(span)
        now = 1 if 3 in span else size
        pick(buffer, range(begin + started, begin + now))
        for part in span:
            arrived(recv_weights, weights_sems.at[part], parts[part][1] - (part == 0))
        pick(buffer, range(begin + now, begin + size))

        started = 0
        if index + 1 < len(spans) and 3 not in span and 3 not in spans[index + 1]:
            wait_ids(spans[index + 1])
            following = parts[spans[index + 1][0]][0]
            started = AHEAD
            pick(1 - buffer, range(following, following + started))
        if 3 in span:
            multiply(buffer, [begin])
            answer([begin])
            begin, size = begin + 1, size - 1
        multiply(buffer, range(begin, begin + size))
        answer(range(begin, begin + size))

    recv_sums[my_batch, my_table] = send_sums[0]
    last = recv_weights[0, pl.ds(2 * halves - 1, 1), :]
    for source in range(1, devices):
        last = jnp.maximum(last, recv_weights[source, pl.ds(2 * halves - 1, 1), :])
    flag_out[...] = jnp.broadcast_to(jnp.max(jnp.where(lane1 == LANES - 1, last, 0)), (LANES,))
    flag_copy = pltpu.make_async_copy(flag_out, flag_ref, local_sems.at[3])
    flag_copy.start()
    scales = []
    for k in range(tables):
        lengths = jnp.zeros((samples, LANES), jnp.int32)
        for bag in range(short_dev):
            lengths = jnp.where(
                sample_rows == short_sample_ref[k, bag], short_len_ref[k, bag], lengths
            )
        for bag in range(long_dev):
            lengths = jnp.where(
                sample_rows == long_sample_ref[bag, k], long_len_ref[bag, k], lengths
            )
        scales.append(jnp.sqrt(lengths.astype(jnp.float32)))

    arrived(send_sums, sums_sem, devices - 1)

    for k in range(tables):
        total = recv_sums[0, k]
        for s in range(1, batch):
            total = total + recv_sums[s, k]
        out_ref[:, k, :] = total / scales[k]

    flag_copy.wait()
    arrived(recv_ids, local_sems.at[0], devices - 1)
    arrived(recv_weights, local_sems.at[1], devices - 1)
    arrived(send_sums, local_sems.at[2], devices - 1)


def choose(index, first, second, *operands):
    branches = tuple(jax.make_jaxpr(branch)(*operands) for branch in (first, second))
    return cond_p.bind(index, *operands, branches=branches)[0]


def on_device(emb, short_rows, short_len, short_sample, long_rows, long_len, long_sample):
    tables = lax.axis_size("table")
    batch = lax.axis_size("batch")
    devices = tables * batch
    short_dev, _, short_width = short_rows.shape
    long_dev, _, long_width = long_rows.shape
    rows_dev, width = emb.shape[1:]
    samples = short_dev + long_dev
    slots = capacity_of(short_dev, short_width, long_dev, long_width, batch)
    halves = pl.cdiv(slots, LANES)
    assert width == LANES and rows_dev <= 65536 and rows_dev % (TABLE_CHUNKS * CONVERT_ROWS) == 0
    assert long_width % LANES == 0 and LANES % short_width == 0
    assert devices % GROUP == 0 and tables & (tables - 1) == 0 and batch & (batch - 1) == 0

    smem = pl.BlockSpec(memory_space=pltpu.SMEM)
    vmem = pl.BlockSpec(memory_space=pltpu.VMEM)
    hbm = pl.BlockSpec(memory_space=pl.ANY)
    call = pl.pallas_call(
        functools.partial(pool_kernel, tables, batch, slots),
        out_shape=(
            jax.ShapeDtypeStruct((samples, tables, width), jnp.float32),
            pltpu.SMEM((128,), jnp.int32),
        ),
        in_specs=[smem] + [hbm] * 7,
        out_specs=(vmem, hbm),
        scratch_shapes=[
            pltpu.VMEM(short_rows.shape, jnp.int32),
            pltpu.SMEM((tables, short_dev), jnp.int32),
            pltpu.SMEM((tables, short_dev), jnp.int32),
            pltpu.VMEM(long_rows.shape, jnp.int32),
            pltpu.SMEM((long_dev, tables), jnp.int32),
            pltpu.SMEM((long_dev, tables), jnp.int32),
            pltpu.VMEM((rows_dev, width), jnp.bfloat16),
            pltpu.VMEM((rows_dev, width), jnp.float32),
            pltpu.VMEM((batch, tables, halves, LANES), jnp.int32),
            pltpu.VMEM((batch, tables, 2 * halves, LANES), jnp.int32),
            pltpu.SMEM((devices, halves, LANES), jnp.int32),
            pltpu.VMEM((devices, 2 * halves, LANES), jnp.int32),
            pltpu.VMEM((2, GROUP, slots, width), jnp.float32),
            pltpu.VMEM((devices, samples, width), jnp.float32),
            pltpu.VMEM((batch, tables, samples, width), jnp.float32),
            pltpu.VMEM((128,), jnp.int32),
            pltpu.SemaphoreType.DMA((INPUTS + TABLE_CHUNKS,)),
            pltpu.SemaphoreType.DMA((devices // GROUP * 2 - 1,)),
            pltpu.SemaphoreType.DMA((devices // GROUP * 2 - 1,)),
            pltpu.SemaphoreType.DMA,
        ],
        compiler_params=pltpu.CompilerParams(
            collective_id=0, has_side_effects=True, vmem_limit_bytes=56 * 2**20
        ),
        name="pool",
    )

    def run(index, operands):
        return call(jnp.reshape(jnp.asarray(index, jnp.int32), (1,)), *operands)

    def rounds(pooled, *operands):
        def again(state):
            index, _, pooled = state
            more, flag = run(index, operands)
            return index + 1, flag[0], pooled + more

        state = (jnp.int32(1), jnp.int32(1), pooled)
        return lax.while_loop(lambda state: state[1] > 0, again, state)[2]

    operands = (emb, short_rows, short_len.T, short_sample.T, long_rows, long_len, long_sample)
    pooled, flag = run(0, operands)
    return choose(flag[0], lambda value, *_: value, rounds, pooled, *operands)


def solution(mesh):
    return jax.shard_map(
        on_device,
        mesh=mesh,
        in_specs=(
            P("table", "batch", None),
            P(("table", "batch"), None, None),
            P(("table", "batch"), None),
            P(("table", "batch"), None),
            P(("table", "batch"), None, None),
            P(("table", "batch"), None),
            P(("table", "batch"), None),
        ),
        out_specs=P(("table", "batch"), None, None),
        check_vma=False,
    )
```
